128 devices in a mesh: grp: 8 (over x, z_lo), mem: 16 (over z_hi, y, core).
Axes of the slice: x: 4, y: 4, z: 4 (z_hi: 2, z_lo: 2; z = z_hi * 2 + z_lo), core: 2. Of those that a mesh axis runs over, the one named last changes fastest.
Arguments:
- weight: bfloat16 [4, 8192, 16384], P(None, None, ('grp', 'mem')), may hold values from -0.046875 to 0.046875
- activation: bfloat16 [2, 16384, 512], P(None, ('grp', 'mem')), may hold values from -6 to 6
- points: int32 [8], replicated, may hold values from 0 to 7, each once
Outputs:
- share: float32 [8, 8192, 512], P('grp', 'mem')
The draws below stay inside these ranges and needn't reach their ends.
Inputs may be any that keep to these rules, and one draw needn't show every extreme that they name: A permutation of 0 to 7; group g evaluates at points[g] + 1.
All inputs are finite; a program needn't handle non-finite values.
Results may differ from the reference program's by a relative error of at most 0.0042.
Values may be sent and summed in bfloat16 or wider, within the bound.
No kernel may reach another device: no remote copies, remote signals or barrier semaphores. Data moves between devices by JAX's collectives and lax.ppermute only.
A program may use at most 320 MiB of HBM per device.

```python
import jax
import jax.numpy as jnp

D = 16384
C = 512
SPLITS = 2
BLOCKS = 4
FB = 8192
N_GRP = 8


def steps_of(own_key, extent, cuts, low, high):
    level = 1.0
    for dim, blocks in cuts:
        steps = jax.random.uniform(jax.random.fold_in(jax.random.fold_in(own_key, 6), dim), (blocks,), jnp.float32, low / len(cuts), high / len(cuts))
        level = level * jnp.repeat(jnp.exp(steps), extent[dim] // blocks).reshape((-1,) + (1,) * (len(extent) - 1 - dim))
    return level


def scatter_about(stream_key, dims, width, bound, cuts=(), held_as=jnp.bfloat16):
    entries = width * jax.random.normal(stream_key, dims, jnp.float32)
    if cuts:
        entries = entries * steps_of(stream_key, dims, cuts, -0.22, 0.18)
    return jnp.clip(entries, -bound, bound).astype(held_as)


def setup_inputs(seed: int = 0) -> dict:
    keys = jax.random.split(jax.random.key(seed), 4)
    weight = scatter_about(keys[0], (BLOCKS, FB, D), D ** -0.5, 0.046875, ((2, 128),))
    activation = scatter_about(keys[1], (SPLITS, D, C), 1.0, 6.0, ((1, 128),))
    points = jax.random.permutation(keys[2], N_GRP).astype(jnp.int32)
    return {"weight": weight, "activation": activation, "points": points}


def reference(weight, activation, points):
    anchors = (points + 1).astype(jnp.float32) / N_GRP
    weight_powers = jnp.arange(BLOCKS, dtype=jnp.float32)
    input_powers = jnp.arange(SPLITS, dtype=jnp.float32) * BLOCKS
    shares = []
    for group in range(N_GRP):
        factors = anchors[group] ** weight_powers
        total = factors[0] * weight[0].astype(jnp.float32)
        for block in range(1, BLOCKS):
            total = total + factors[block] * weight[block].astype(jnp.float32)
        coded_weight = total.astype(jnp.bfloat16)
        lifts = anchors[group] ** input_powers
        mixed = lifts[0] * activation[0].astype(jnp.float32)
        for split in range(1, SPLITS):
            mixed = mixed + lifts[split] * activation[split].astype(jnp.float32)
        coded_input = mixed.astype(jnp.bfloat16)
        shares.append(jnp.dot(coded_weight, coded_input, preferred_element_type=jnp.float32))
    return jnp.stack(shares)
```

```python
import functools

import jax
import jax.numpy as jnp
import numpy as np
from jax import lax
from jax.experimental import pallas as pl
from jax.experimental.pallas import tpu as pltpu
from jax.sharding import Mesh
from jax.sharding import PartitionSpec as P


AXES = ("x", "zl", "zh", "y", "c")
SIZES = {"x": 4, "zl": 2, "zh": 2, "y": 4, "c": 2}
TOKENS = 512
ROWS_X, ROWS_Y, ROWS_Z = 128, 192, 192
AT_Y, AT_Z = ROWS_X, ROWS_X + ROWS_Y
VMEM = pl.BlockSpec(memory_space=pltpu.VMEM)
SMEM = pl.BlockSpec(memory_space=pltpu.SMEM)
ANY = pl.BlockSpec(memory_space=pl.ANY)
F32, BF16 = jnp.float32, jnp.bfloat16


def flip(value, axis, d, dc=0):
    over = [n for n in AXES if (n == "c" and dc) or (d and (n == axis or (axis == "z" and n in ("zl", "zh"))))]
    sizes = [SIZES[n] for n in over]
    pairs = []
    for i in range(int(np.prod(sizes))):
        at = dict(zip(over, (int(k) for k in np.unravel_index(i, sizes))))
        to = dict(at)
        if d and axis == "z":
            to["zl"] ^= d & 1
            to["zh"] ^= d >> 1
        elif d:
            to[axis] ^= d
        if dc:
            to["c"] ^= 1
        pairs.append((i, int(np.ravel_multi_index([to[n] for n in over], sizes))))
    return lax.ppermute(value, tuple(over), pairs)


def source_slices(family, w, where, d, dc):
    x, y, zl, zh, c = (where[i] for i in range(5))
    c = c ^ dc
    if family == "x":
        return w.at[:, :, :, c, pl.ds(pl.multiple_of((x ^ d) * (ROWS_X // 4), 16), ROWS_X // 4), :]
    if family == "y":
        return w.at[:, :, y ^ d, c, pl.ds(AT_Y, ROWS_Y), :]
    start = pl.multiple_of(AT_Z + (zl ^ (d & 1)) * (ROWS_Z // 2), 16)
    return w.at[:, zh ^ (d >> 1), :, c, pl.ds(start, ROWS_Z // 2), :]


PIECE = {
    "x": (4, 2, 4, ROWS_X // 4, 128),
    "y": (4, 2, ROWS_Y, 128),
    "z": (4, 4, ROWS_Z // 2, 128),
}
SOURCES = tuple((d, dc) for dc in (0, 1) for d in range(4))


def pack_kernel(family, where, w, *refs):
    outs, sem = refs[:8], refs[8]
    copies = [
        pltpu.make_async_copy(source_slices(family, w, where, d, dc), out, sem.at[i])
        for i, ((d, dc), out) in enumerate(zip(SOURCES, outs))
    ]
    for copy in copies:
        copy.start()
    for copy in copies:
        copy.wait()


def pack(family, weight, where):
    shape = PIECE[family]
    size = int(np.prod(shape)) * 2
    return pl.pallas_call(
        functools.partial(pack_kernel, family),
        out_shape=[jax.ShapeDtypeStruct(shape, BF16)] * 8,
        in_specs=[SMEM, ANY],
        out_specs=[VMEM] * 8,
        scratch_shapes=[pltpu.SemaphoreType.DMA((8,))],
        cost_estimate=pl.CostEstimate(flops=0, bytes_accessed=16 * size, transcendentals=0),
        name=f"pack_{family}",
    )(where, weight)


def plan_of(family, where):
    x, y, zl, zh = (where[i] for i in range(4))
    if family == "y":
        sends = [(d, gz, ((x ^ d) * 2 + gz)) for d in range(4) for gz in range(2)]
        return [(0, 2 * ROWS_Y, sends)]
    if family == "z":
        return [((y ^ d) * (ROWS_Z // 2), ROWS_Z // 2, [(d, g, g) for g in range(8)]) for d in range(4)]
    return [
        ((zh ^ e) * ROWS_X, ROWS_X, [(2 * e + f, gx, gx * 2 + (zl ^ f)) for f in range(2) for gx in range(4)])
        for e in range(2)
    ]


OUT = {"x": (4, ROWS_X, TOKENS), "y": (2, 2 * ROWS_Y, TOKENS), "z": (8, ROWS_Z // 2, TOKENS)}
TILE = {"x": 64, "y": 64, "z": 48}


def product_kernel(family, where, factors, *refs):
    w, xs, xd = refs[:8], refs[8:12], refs[12]
    outs, xcat, prod = refs[13:17], refs[17], refs[18]
    for s in range(8):
        for k in range(2):
            piece = xs[s][k] if s < 4 else xd[s - 4, k]
            xcat[s * 128 : (s + 1) * 128, k * TOKENS : (k + 1) * TOKENS] = piece
    tile = TILE[family]
    for start, rows, sends in plan_of(family, where):

        @pl.loop(0, rows // tile)
        def _(t):
            at = pl.multiple_of(start + t * tile, 16)
            for j in range(4):
                left = jnp.concatenate([w[s][j, pl.ds(at, tile), :] for s in range(8)], axis=1)
                prod[j] = jnp.dot(left, xcat[...], preferred_element_type=F32)

            @pl.loop(0, tile // 16)
            def _(r):
                here = pl.ds(pl.multiple_of(r * 16, 16), 16)
                there = pl.ds(pl.multiple_of(t * tile + r * 16, 16), 16)
                for col in range(0, TOKENS, 256):
                    terms = [prod[p % 4, here, pl.ds((p // 4) * TOKENS + col, 256)] for p in range(8)]
                    for d, slot, group in sends:
                        total = terms[0]
                        for p in range(1, 8):
                            total = total + factors[group * 8 + p] * terms[p]
                        outs[d][slot, there, pl.ds(col, 256)] = total.astype(BF16)


def product(family, pieces, xs, xd, where, factors):
    rows = int(np.prod(PIECE[family][1:-1]))
    pieces = [p.reshape(4, rows, 128) for p in pieces]
    flops = 2 * 4 * rows * 1024 * 1024
    return pl.pallas_call(
        functools.partial(product_kernel, family),
        out_shape=[jax.ShapeDtypeStruct(OUT[family], BF16)] * 4,
        in_specs=[SMEM, SMEM] + [VMEM] * 13,
        out_specs=[VMEM] * 4,
        scratch_shapes=[pltpu.VMEM((1024, 1024), BF16), pltpu.VMEM((4, TILE[family], 1024), F32)],
        cost_estimate=pl.CostEstimate(flops=2 * flops, bytes_accessed=8 << 20, transcendentals=0),
        compiler_params=pltpu.CompilerParams(vmem_limit_bytes=40 << 20),
        name=f"product_{family}",
    )(where, factors, *pieces, *xs, xd)


def cut_kernel(index, where, *refs):
    parts, outs = refs[:4], refs[4:]
    pos = tuple(where[i] for i in range(4))
    for d, out in enumerate(outs):
        at = index(pos, d)
        total = parts[0][at].astype(F32)
        for part in parts[1:]:
            total = total + part[at].astype(F32)
        out[...] = total.astype(out.dtype)


def sum_and_cut(name, parts, where, index, shape, sends):
    size = int(np.prod(parts[0].shape))
    return pl.pallas_call(
        functools.partial(cut_kernel, index),
        out_shape=[jax.ShapeDtypeStruct(shape, F32)] + [jax.ShapeDtypeStruct(shape, BF16)] * sends,
        in_specs=[SMEM] + [VMEM] * 4,
        out_specs=[VMEM] * (sends + 1),
        cost_estimate=pl.CostEstimate(flops=size * 4, bytes_accessed=size * 12, transcendentals=0),
        name=name,
    )(where, *parts)


def exchange(parts, axis):
    return [parts[0]] + [flip(parts[d], axis, d) for d in range(1, len(parts))]


def final_kernel(where, *refs):
    fx, fy, fz, out = refs[:4], refs[4:8], refs[8:10], refs[10]
    x, zl = where[0], where[2]
    quarter, half = ROWS_X // 4, ROWS_Z // 2
    for d in range(4):
        out[0, pl.ds(pl.multiple_of((x ^ d) * quarter, 16), quarter), :] = fx[d][...].astype(F32)
    total = fy[0][...]
    for part in fy[1:]:
        total = total + part[...].astype(F32)
    out[0, AT_Y : AT_Y + ROWS_Y, :] = total
    for d in range(2):
        out[0, pl.ds(pl.multiple_of(AT_Z + (zl ^ d) * half, 16), half), :] = fz[d][...].astype(F32)


def per_device(weight, activation, points):
    x, y, c = lax.axis_index("x"), lax.axis_index("y"), lax.axis_index("c")
    zl, zh = lax.axis_index("zl"), lax.axis_index("zh")
    where = jnp.stack([x, y, zl, zh, c]).astype(jnp.int32)
    anchors = (points + 1).astype(F32) / 8
    powers = jnp.arange(4, dtype=F32)
    low = anchors[:, None] ** powers[None, :]
    high = anchors[:, None] ** (4 * jnp.arange(2, dtype=F32))[None, :]
    factors = (high[:, :, None] * low[:, None, :]).reshape(64)
    view = weight.reshape(4, 2, 4, 2, 512, 128)

    xs, pieces = {}, {}
    for family in "xyz":
        xs[family] = exchange([activation] * 4, family)
    for family in "xyz":
        sent = pack(family, view, where)
        pieces[family] = [flip(p, family, d, dc) if d or dc else p for (d, dc), p in zip(SOURCES, sent)]
    parts = {}
    for family in "xyz":
        xd = flip(jnp.stack(xs[family]), "c", 0, 1)
        parts[family] = product(family, pieces[family], xs[family], xd, where, factors)

    px = [p.reshape(4, 4, ROWS_X // 4, TOKENS) for p in exchange(parts["x"], "z")]
    py = [p.reshape(2, 2, ROWS_Y, TOKENS) for p in exchange(parts["y"], "x")]
    pz = [p.reshape(4, 2, ROWS_Z // 2, TOKENS) for p in exchange(parts["z"], "y")]
    px = sum_and_cut(
        "sum1_x", px, where, lambda pos, d: (slice(None), pos[1] ^ d), (4, ROWS_X // 4, TOKENS), 3)
    py = sum_and_cut(
        "sum1_y", py, where, lambda pos, d: (pos[2] ^ (d & 1), pos[3] ^ (d >> 1)), (ROWS_Y, TOKENS), 3)
    pz = sum_and_cut("sum1_z", pz, where, lambda pos, d: (pos[0] ^ d,), (2, ROWS_Z // 2, TOKENS), 3)
    px, py, pz = exchange(px, "y"), exchange(py, "z"), exchange(pz, "x")
    px = sum_and_cut("sum2_x", px, where, lambda pos, d: (pos[0] ^ d,), (ROWS_X // 4, TOKENS), 3)
    pz = sum_and_cut("sum2_z", pz, where, lambda pos, d: (pos[2] ^ d,), (ROWS_Z // 2, TOKENS), 1)
    px, pz = exchange(px, "x"), exchange(pz, "z")
    return pl.pallas_call(
        final_kernel,
        out_shape=jax.ShapeDtypeStruct((1, 512, TOKENS), F32),
        in_specs=[SMEM] + [VMEM] * 10,
        out_specs=VMEM,
        cost_estimate=pl.CostEstimate(flops=1 << 20, bytes_accessed=3 << 20, transcendentals=0),
        name="final",
    )(where, *px, *py, *pz)


def solution(mesh):
    split = Mesh(mesh.devices.reshape(4, 2, 2, 4, 2), AXES)
    grp, mem = ("x", "zl"), ("zh", "y", "c")
    placed = (P(None, None, grp + mem), P(None, grp + mem, None), P())
    return jax.shard_map(
        per_device, mesh=split, in_specs=placed, out_specs=P(grp, mem, None), check_vma=False
    )
```

```python
import functools

import jax
import jax.numpy as jnp
import numpy as np
from jax import lax
from jax.experimental import pallas as pl
from jax.experimental.pallas import tpu as pltpu
from jax.sharding import Mesh
from jax.sharding import PartitionSpec as P


AXES = ("x", "zl", "zh", "y", "c")
SIZES = {"x": 4, "zl": 2, "zh": 2, "y": 4, "c": 2}
TOKENS = 512
FAMILIES = "yzx"
ROWS_X, ROWS_Y, ROWS_Z = 128, 192, 192
AT_Y, AT_Z = ROWS_X, ROWS_X + ROWS_Y
VMEM = pl.BlockSpec(memory_space=pltpu.VMEM)
SMEM = pl.BlockSpec(memory_space=pltpu.SMEM)
ANY = pl.BlockSpec(memory_space=pl.ANY)
HBM = pl.BlockSpec(memory_space=pltpu.HBM)
F32, BF16 = jnp.float32, jnp.bfloat16


def flip(value, axis, d, dc=0):
    over = [n for n in AXES if (n == "c" and dc) or (d and (n == axis or (axis == "z" and n in ("zl", "zh"))))]
    sizes = [SIZES[n] for n in over]
    pairs = []
    for i in range(int(np.prod(sizes))):
        at = dict(zip(over, (int(k) for k in np.unravel_index(i, sizes))))
        to = dict(at)
        if d and axis == "z":
            to["zl"] ^= d & 1
            to["zh"] ^= d >> 1
        elif d:
            to[axis] ^= d
        if dc:
            to["c"] ^= 1
        pairs.append((i, int(np.ravel_multi_index([to[n] for n in over], sizes))))
    return lax.ppermute(value, tuple(over), pairs)


def source_slices(family, w, where, d, dc):
    x, y, zl, zh, c = (where[i] for i in range(5))
    c = c ^ dc
    if family == "x":
        return w.at[:, :, :, c, pl.ds(pl.multiple_of((x ^ d) * (ROWS_X // 4), 16), ROWS_X // 4), :]
    if family == "y":
        return w.at[:, :, y ^ d, c, pl.ds(AT_Y, ROWS_Y), :]
    start = pl.multiple_of(AT_Z + (zl ^ (d & 1)) * (ROWS_Z // 2), 16)
    return w.at[:, zh ^ (d >> 1), :, c, pl.ds(start, ROWS_Z // 2), :]


PIECE = {
    "x": (4, 2, 4, ROWS_X // 4, 128),
    "y": (4, 2, ROWS_Y, 128),
    "z": (4, 4, ROWS_Z // 2, 128),
}
SOURCES = tuple((d, dc) for dc in (0, 1) for d in range(4))
CHUNK = 32
FEATURES = 2 * 4 * 128


def rows_of(family):
    return int(np.prod(PIECE[family][1:-1]))


def planes_of(family):
    return 8 + -(-FEATURES // rows_of(family))


def plane_at(shape, row):
    index, at = [], row
    for n in shape[::-1]:
        index.append(at % n)
        at //= n
    return (at, *index[:0:-1], pl.ds(index[0], CHUNK))


def pack_kernel(family, where, w, act, *refs):
    outs, token, xstage, xin, sem, x_sem = refs[:4], refs[4], *refs[5:]
    read = pltpu.make_async_copy(act, xin, x_sem.at[0])
    read.start()
    copies = [
        pltpu.make_async_copy(source_slices(family, w, where, d, dc), outs[d].at[pl.ds(4 * dc, 4)], sem.at[i])
        for i, (d, dc) in enumerate(SOURCES)
    ]
    for copy in copies:
        copy.start()
    for i in range(5):
        token[i] = where[i]
    read.wait()
    for k in range(2):
        for ct in range(4):
            for r in range(0, 128, CHUNK):
                at = plane_at(PIECE[family][1:-1], (k * 4 + ct) * 128 + r)
                xstage[at] = xin[k, r : r + CHUNK, ct * 128 : (ct + 1) * 128]
    writes = [
        pltpu.make_async_copy(xstage, out.at[pl.ds(8, xstage.shape[0])], x_sem.at[i]) for i, out in enumerate(outs)
    ]
    for write in writes:
        write.start()
    for copy in copies + writes:
        copy.wait()


def pack(family, weight, act, where):
    shape = PIECE[family]
    wide = (planes_of(family), *shape[1:])
    size = int(np.prod(shape)) * 2
    out = pl.pallas_call(
        functools.partial(pack_kernel, family),
        out_shape=[jax.ShapeDtypeStruct(wide, BF16)] * 4 + [jax.ShapeDtypeStruct((5,), jnp.int32)],
        in_specs=[SMEM, HBM, HBM],
        out_specs=[ANY] * 4 + [SMEM],
        scratch_shapes=[
            pltpu.VMEM((wide[0] - 8, *shape[1:]), BF16),
            pltpu.VMEM(act.shape, BF16),
            pltpu.SemaphoreType.DMA((8,)),
            pltpu.SemaphoreType.DMA((4,)),
        ],
        cost_estimate=pl.CostEstimate(flops=0, bytes_accessed=16 * size, transcendentals=0),
        compiler_params=pltpu.CompilerParams(vmem_limit_bytes=4 << 20),
    )(where, weight, act)
    return out[:4], out[4]


def relay_kernel(order, *refs):
    pieces, out, token, sem = refs[:4], refs[4], refs[5], refs[6]
    copies = [pltpu.make_async_copy(p.at[pl.ds(4, out.shape[1])], out.at[i], sem.at[i]) for i, p in enumerate(pieces)]
    for copy in copies:
        copy.start()
    token[0] = order[0]
    for copy in copies:
        copy.wait()


def relay(family, pieces, order):
    shape = (4, planes_of(family) - 4, *PIECE[family][1:])
    return pl.pallas_call(
        relay_kernel,
        out_shape=[jax.ShapeDtypeStruct(shape, BF16), jax.ShapeDtypeStruct((1,), jnp.int32)],
        in_specs=[SMEM] + [ANY] * 4,
        out_specs=[VMEM, SMEM],
        scratch_shapes=[pltpu.SemaphoreType.DMA((4,))],
        cost_estimate=pl.CostEstimate(flops=0, bytes_accessed=4 << 20, transcendentals=0),
        compiler_params=pltpu.CompilerParams(vmem_limit_bytes=5 << 20),
    )(order, *pieces)


def plan_of(family, where):
    x, y, zl, zh = (where[i] for i in range(4))
    if family == "y":
        sends = [(d, gz, ((x ^ d) * 2 + gz)) for d in range(4) for gz in range(2)]
        return [(t * 96, 96, t * 96, sends) for t in range(4)]
    if family == "z":
        return [((y ^ d) * 96, 96, 0, [(d, g, g) for g in range(8)]) for d in range(4)]
    return [
        ((zh ^ e) * ROWS_X + t * 64, 64, t * 64,
         [(2 * e + f, gx, gx * 2 + (zl ^ f)) for f in range(2) for gx in range(4)])
        for e in range(2) for t in range(2)
    ]


OUT = {"x": (4, ROWS_X, TOKENS), "y": (2, 2 * ROWS_Y, TOKENS), "z": (8, ROWS_Z // 2, TOKENS)}
TILE = {"x": 64, "y": 96, "z": 96}


def product_kernel(family, where, factors, order, *refs):
    own, shared = refs[:4], refs[4]
    outs, token, xcat, prods = refs[5:9], refs[9], refs[10], refs[11:13]
    w = [*own, *(shared.at[d] for d in range(4))]
    token[0] = order[0]
    rows, tile = rows_of(family), TILE[family]
    for s in range(8):
        for k in range(2):
            for ct in range(4):
                for r in range(0, 128, CHUNK):
                    at = plane_at((rows,), (k * 4 + ct) * 128 + r)
                    at = (at[0] + (8 if s < 4 else 4), *at[1:])
                    piece = w[s][at]
                    xcat[s * 128 + r : s * 128 + r + CHUNK, k * TOKENS + ct * 128 : k * TOKENS + (ct + 1) * 128] = piece
    plan = plan_of(family, where)

    def multiply(start, prod):
        here = pl.ds(start if isinstance(start, int) else pl.multiple_of(start, 16), tile)
        left = [jnp.concatenate([w[s][j, here, :] for s in range(8)], axis=1) for j in range(4)]
        prod[...] = jnp.dot(jnp.concatenate(left, axis=0), xcat[...], preferred_element_type=F32)

    anchors = [factors[g] for g in range(8)] if family == "z" else None

    def combine(first, sends, prod):
        at = anchors or [factors[group] for _, _, group in sends]
        for r in range(0, tile, 8):
            for col in range(0, TOKENS, 256):
                terms = [
                    prod[(p % 4) * tile + r : (p % 4) * tile + r + 8, (p // 4) * TOKENS + col : (p // 4) * TOKENS + col + 256]
                    for p in range(8)
                ]
                for (d, slot, _), anchor in zip(sends, at):
                    total = terms[7]
                    for p in range(6, -1, -1):
                        total = total * anchor + terms[p]
                    outs[d][slot, first + r : first + r + 8, col : col + 256] = total.astype(BF16)

    multiply(plan[0][0], prods[0])
    for t in range(4):
        if t < 3:
            multiply(plan[t + 1][0], prods[(t + 1) % 2])
        combine(plan[t][2], plan[t][3], prods[t % 2])


def product(family, pieces, shared, where, factors, order):
    rows = rows_of(family)
    planes = planes_of(family)
    pieces = [p.reshape(-1, rows, 128) for p in pieces]
    shared = shared.reshape(4, planes - 4, rows, 128)
    flops = 2 * 4 * rows * 1024 * 1024
    out = pl.pallas_call(
        functools.partial(product_kernel, family),
        out_shape=[jax.ShapeDtypeStruct(OUT[family], BF16)] * 4 + [jax.ShapeDtypeStruct((1,), jnp.int32)],
        in_specs=[SMEM, SMEM, SMEM] + [VMEM] * 5,
        out_specs=[VMEM] * 4 + [SMEM],
        scratch_shapes=[pltpu.VMEM((1024, 1024), BF16)] + [pltpu.VMEM((4 * TILE[family], 1024), F32)] * 2,
        cost_estimate=pl.CostEstimate(flops=2 * flops, bytes_accessed=8 << 20, transcendentals=0),
        compiler_params=pltpu.CompilerParams(vmem_limit_bytes=22 << 20),
    )(where, factors, order, *pieces, shared)
    return out[:4], out[4]


def cut_kernel(index, where, *refs):
    parts, outs = refs[:4], refs[4:]
    pos = tuple(where[i] for i in range(4))
    for d, out in enumerate(outs):
        at = index(pos, d)
        total = parts[0][at].astype(F32)
        for part in parts[1:]:
            total = total + part[at].astype(F32)
        out[...] = total.astype(out.dtype)


def sum_and_cut(parts, where, index, shape, sends):
    size = int(np.prod(parts[0].shape))
    return pl.pallas_call(
        functools.partial(cut_kernel, index),
        out_shape=[jax.ShapeDtypeStruct(shape, F32)] + [jax.ShapeDtypeStruct(shape, BF16)] * sends,
        in_specs=[SMEM] + [VMEM] * 4,
        out_specs=[VMEM] * (sends + 1),
        cost_estimate=pl.CostEstimate(flops=size * 4, bytes_accessed=size * 12, transcendentals=0),
        compiler_params=pltpu.CompilerParams(vmem_limit_bytes=8 << 20),
    )(where, *parts)


def exchange(parts, axis):
    return [parts[0]] + [flip(parts[d], axis, d) for d in range(1, len(parts))]


def final_kernel(where, *refs):
    fx, fy, fz, out = refs[:4], refs[4:8], refs[8:10], refs[10]
    x, zl = where[0], where[2]
    quarter, half = ROWS_X // 4, ROWS_Z // 2
    for d in range(4):
        out[0, pl.ds(pl.multiple_of((x ^ d) * quarter, 16), quarter), :] = fx[d][...].astype(F32)
    total = fy[0][...]
    for part in fy[1:]:
        total = total + part[...].astype(F32)
    out[0, AT_Y : AT_Y + ROWS_Y, :] = total
    for d in range(2):
        out[0, pl.ds(pl.multiple_of(AT_Z + (zl ^ d) * half, 16), half), :] = fz[d][...].astype(F32)


def per_device(weight, activation, points):
    x, y, c = lax.axis_index("x"), lax.axis_index("y"), lax.axis_index("c")
    zl, zh = lax.axis_index("zl"), lax.axis_index("zh")
    where = jnp.stack([x, y, zl, zh, c]).astype(jnp.int32)
    factors = (points + 1).astype(F32) / 8
    view = weight.reshape(4, 2, 4, 2, 512, 128)

    pieces, parts, order = {}, {}, where
    for family in FAMILIES:
        sent, order = pack(family, view, activation, order)
        pieces[family] = exchange(sent, family)
    order, shared = order[:1], {}

    def share(family, order):
        xd, order = relay(family, pieces[family], order)
        shared[family] = flip(xd, "c", 0, 1)
        return order

    order = share(FAMILIES[0], order)
    for family, after in zip(FAMILIES, (*FAMILIES[1:], None)):
        if after:
            order = share(after, order)
        parts[family], order = product(family, pieces[family], shared[family], where, factors, order)

    px = exchange(parts["x"], "z")
    py = exchange(parts["y"], "x")
    pz = exchange(parts["z"], "y")
    px = [p.reshape(4, 4, ROWS_X // 4, TOKENS) for p in px]
    py = [p.reshape(2, 2, ROWS_Y, TOKENS) for p in py]
    pz = [p.reshape(4, 2, ROWS_Z // 2, TOKENS) for p in pz]
    px = sum_and_cut(
        px, where, lambda pos, d: (slice(None), pos[1] ^ d), (4, ROWS_X // 4, TOKENS), 3)
    py = sum_and_cut(
        py, where, lambda pos, d: (pos[2] ^ (d & 1), pos[3] ^ (d >> 1)), (ROWS_Y, TOKENS), 3)
    pz = sum_and_cut(pz, where, lambda pos, d: (pos[0] ^ d,), (2, ROWS_Z // 2, TOKENS), 3)
    px = exchange(px, "y")
    py = exchange(py, "z")
    pz = exchange(pz, "x")
    px = sum_and_cut(px, where, lambda pos, d: (pos[0] ^ d,), (ROWS_X // 4, TOKENS), 3)
    pz = sum_and_cut(pz, where, lambda pos, d: (pos[2] ^ d,), (ROWS_Z // 2, TOKENS), 1)
    px = exchange(px, "x")
    pz = exchange(pz, "z")
    return pl.pallas_call(
        final_kernel,
        out_shape=jax.ShapeDtypeStruct((1, 512, TOKENS), F32),
        in_specs=[SMEM] + [VMEM] * 10,
        out_specs=VMEM,
        cost_estimate=pl.CostEstimate(flops=1 << 20, bytes_accessed=3 << 20, transcendentals=0),
        compiler_params=pltpu.CompilerParams(vmem_limit_bytes=8 << 20),
        name="final",
    )(where, *px, *py, *pz)


def solution(mesh):
    split = Mesh(mesh.devices.reshape(4, 2, 2, 4, 2), AXES)
    grp, mem = ("x", "zl"), ("zh", "y", "c")
    placed = (P(None, None, grp + mem), P(None, grp + mem, None), P())
    return jax.shard_map(per_device, mesh=split, in_specs=placed, out_specs=P(grp, mem, None), check_vma=False)
```

```python
import functools

import jax
import jax.numpy as jnp
import numpy as np
from jax import lax
from jax.experimental import pallas as pl
from jax.experimental.pallas import tpu as pltpu
from jax.sharding import Mesh
from jax.sharding import PartitionSpec as P


AXES = ("x", "zl", "zh", "y", "c")
SIZES = {"x": 4, "zl": 2, "zh": 2, "y": 4, "c": 2}
TOKENS = 512
FAMILIES = "yzx"
ROWS_X, ROWS_Y, ROWS_Z = 128, 192, 192
AT_Y, AT_Z = ROWS_X, ROWS_X + ROWS_Y
VMEM = pl.BlockSpec(memory_space=pltpu.VMEM)
SMEM = pl.BlockSpec(memory_space=pltpu.SMEM)
ANY = pl.BlockSpec(memory_space=pl.ANY)
HBM = pl.BlockSpec(memory_space=pltpu.HBM)
F32, BF16 = jnp.float32, jnp.bfloat16


def flip(value, axis, d, dc=0):
    over = [n for n in AXES if (n == "c" and dc) or (d and (n == axis or (axis == "z" and n in ("zl", "zh"))))]
    sizes = [SIZES[n] for n in over]
    pairs = []
    for i in range(int(np.prod(sizes))):
        at = dict(zip(over, (int(k) for k in np.unravel_index(i, sizes))))
        to = dict(at)
        if d and axis == "z":
            to["zl"] ^= d & 1
            to["zh"] ^= d >> 1
        elif d:
            to[axis] ^= d
        if dc:
            to["c"] ^= 1
        pairs.append((i, int(np.ravel_multi_index([to[n] for n in over], sizes))))
    return lax.ppermute(value, tuple(over), pairs)


def source_slices(family, w, where, d, dc):
    x, y, zl, zh, c = (where[i] for i in range(5))
    c = c ^ dc
    if family == "x":
        return w.at[:, :, :, c, pl.ds(pl.multiple_of((x ^ d) * (ROWS_X // 4), 16), ROWS_X // 4), :]
    if family == "y":
        return w.at[:, :, y ^ d, c, pl.ds(AT_Y, ROWS_Y), :]
    start = pl.multiple_of(AT_Z + (zl ^ (d & 1)) * (ROWS_Z // 2), 16)
    return w.at[:, zh ^ (d >> 1), :, c, pl.ds(start, ROWS_Z // 2), :]


PIECE = {
    "x": (4, 2, 4, ROWS_X // 4, 128),
    "y": (4, 2, ROWS_Y, 128),
    "z": (4, 4, ROWS_Z // 2, 128),
}
SOURCES = tuple((d, dc) for dc in (0, 1) for d in range(4))
CHUNK = 32
FEATURES = 2 * 4 * 128


def rows_of(family):
    return int(np.prod(PIECE[family][1:-1]))


def planes_of(family):
    return 4 + -(-FEATURES // rows_of(family))


def plane_at(shape, row):
    index, at = [], row
    for n in shape[::-1]:
        index.append(at % n)
        at //= n
    return (4 + at, *index[:0:-1], pl.ds(index[0], CHUNK))


def pack_kernel(family, where, w, act, *refs):
    outs, token, xstage, xin, sem, x_sem = refs[:8], refs[8], *refs[9:]
    read = pltpu.make_async_copy(act, xin, x_sem.at[0])
    read.start()
    copies = [
        pltpu.make_async_copy(
            source_slices(family, w, where, d, dc), out if dc else out.at[pl.ds(0, 4)], sem.at[i]
        )
        for i, ((d, dc), out) in enumerate(zip(SOURCES, outs))
    ]
    for copy in copies:
        copy.start()
    for i in range(5):
        token[i] = where[i]
    read.wait()
    for k in range(2):
        for ct in range(4):
            for r in range(0, 128, CHUNK):
                at = plane_at(PIECE[family][1:-1], (k * 4 + ct) * 128 + r)
                xstage[(at[0] - 4, *at[1:])] = xin[k, r : r + CHUNK, ct * 128 : (ct + 1) * 128]
    writes = [
        pltpu.make_async_copy(xstage, out.at[pl.ds(4, xstage.shape[0])], x_sem.at[i]) for i, out in enumerate(outs[:4])
    ]
    for write in writes:
        write.start()
    for copy in copies + writes:
        copy.wait()


def pack(family, weight, act, where):
    shape = PIECE[family]
    wide = (planes_of(family), *shape[1:])
    size = int(np.prod(shape)) * 2
    shapes = [jax.ShapeDtypeStruct(wide, BF16)] * 4 + [jax.ShapeDtypeStruct(shape, BF16)] * 4
    out = pl.pallas_call(
        functools.partial(pack_kernel, family),
        out_shape=shapes + [jax.ShapeDtypeStruct((5,), jnp.int32)],
        in_specs=[SMEM, HBM, HBM],
        out_specs=[ANY] * 8 + [SMEM],
        scratch_shapes=[
            pltpu.VMEM((wide[0] - 4, *shape[1:]), BF16),
            pltpu.VMEM(act.shape, BF16),
            pltpu.SemaphoreType.DMA((8,)),
            pltpu.SemaphoreType.DMA((4,)),
        ],
        cost_estimate=pl.CostEstimate(flops=0, bytes_accessed=16 * size, transcendentals=0),
        compiler_params=pltpu.CompilerParams(vmem_limit_bytes=4 << 20),
    )(where, weight, act)
    return out[:8], out[8]


def relay_kernel(order, *refs):
    pieces, out, token, sem = refs[:4], refs[4], refs[5], refs[6]
    copies = [pltpu.make_async_copy(p.at[pl.ds(4, out.shape[1])], out.at[i], sem.at[i]) for i, p in enumerate(pieces)]
    for copy in copies:
        copy.start()
    token[0] = order[0]
    for copy in copies:
        copy.wait()


def relay(family, pieces, order):
    shape = (4, planes_of(family) - 4, *PIECE[family][1:])
    return pl.pallas_call(
        relay_kernel,
        out_shape=[jax.ShapeDtypeStruct(shape, BF16), jax.ShapeDtypeStruct((1,), jnp.int32)],
        in_specs=[SMEM] + [ANY] * 4,
        out_specs=[VMEM, SMEM],
        scratch_shapes=[pltpu.SemaphoreType.DMA((4,))],
        cost_estimate=pl.CostEstimate(flops=0, bytes_accessed=4 << 20, transcendentals=0),
        compiler_params=pltpu.CompilerParams(vmem_limit_bytes=4 << 20),
    )(order, *pieces)


def plan_of(family, where):
    x, y, zl, zh = (where[i] for i in range(4))
    if family == "y":
        sends = [(d, gz, ((x ^ d) * 2 + gz)) for d in range(4) for gz in range(2)]
        return [(t * 96, 96, t * 96, sends) for t in range(4)]
    if family == "z":
        return [((y ^ d) * 96, 96, 0, [(d, g, g) for g in range(8)]) for d in range(4)]
    return [
        ((zh ^ e) * ROWS_X + t * 64, 64, t * 64,
         [(2 * e + f, gx, gx * 2 + (zl ^ f)) for f in range(2) for gx in range(4)])
        for e in range(2) for t in range(2)
    ]


OUT = {"x": (4, ROWS_X, TOKENS), "y": (2, 2 * ROWS_Y, TOKENS), "z": (8, ROWS_Z // 2, TOKENS)}
TILE = {"x": 64, "y": 96, "z": 96}


def product_kernel(family, where, factors, order, *refs):
    w, xd = refs[:8], refs[8]
    outs, token, xcat, prods = refs[9:13], refs[13], refs[14], refs[15:17]
    token[0] = order[0]
    rows, tile = rows_of(family), TILE[family]
    for s in range(8):
        for k in range(2):
            for ct in range(4):
                for r in range(0, 128, CHUNK):
                    at = plane_at((rows,), (k * 4 + ct) * 128 + r)
                    piece = w[s][at] if s < 4 else xd[(s - 4, at[0] - 4, *at[1:])]
                    xcat[s * 128 + r : s * 128 + r + CHUNK, k * TOKENS + ct * 128 : k * TOKENS + (ct + 1) * 128] = piece
    plan = plan_of(family, where)

    def multiply(start, prod):
        here = pl.ds(start if isinstance(start, int) else pl.multiple_of(start, 16), tile)
        left = [jnp.concatenate([w[s][j, here, :] for s in range(8)], axis=1) for j in range(4)]
        prod[...] = jnp.dot(jnp.concatenate(left, axis=0), xcat[...], preferred_element_type=F32)

    anchors = [factors[g] for g in range(8)] if family == "z" else None

    def combine(first, sends, prod):
        at = anchors or [factors[group] for _, _, group in sends]
        for r in range(0, tile, 8):
            for col in range(0, TOKENS, 256):
                terms = [
                    prod[(p % 4) * tile + r : (p % 4) * tile + r + 8, (p // 4) * TOKENS + col : (p // 4) * TOKENS + col + 256]
                    for p in range(8)
                ]
                for (d, slot, _), anchor in zip(sends, at):
                    total = terms[7]
                    for p in range(6, -1, -1):
                        total = total * anchor + terms[p]
                    outs[d][slot, first + r : first + r + 8, col : col + 256] = total.astype(BF16)

    multiply(plan[0][0], prods[0])
    for t in range(4):
        if t < 3:
            multiply(plan[t + 1][0], prods[(t + 1) % 2])
        combine(plan[t][2], plan[t][3], prods[t % 2])


def product(family, pieces, xd, where, factors, order):
    rows = rows_of(family)
    planes = planes_of(family)
    pieces = [p.reshape(-1, rows, 128) for p in pieces]
    xd = xd.reshape(4, planes - 4, rows, 128)
    flops = 2 * 4 * rows * 1024 * 1024
    out = pl.pallas_call(
        functools.partial(product_kernel, family),
        out_shape=[jax.ShapeDtypeStruct(OUT[family], BF16)] * 4 + [jax.ShapeDtypeStruct((1,), jnp.int32)],
        in_specs=[SMEM, SMEM, SMEM] + [VMEM] * 9,
        out_specs=[VMEM] * 4 + [SMEM],
        scratch_shapes=[pltpu.VMEM((1024, 1024), BF16)] + [pltpu.VMEM((4 * TILE[family], 1024), F32)] * 2,
        cost_estimate=pl.CostEstimate(flops=2 * flops, bytes_accessed=8 << 20, transcendentals=0),
        compiler_params=pltpu.CompilerParams(vmem_limit_bytes=22 << 20),
    )(where, factors, order, *pieces, xd)
    return out[:4], out[4]


def cut_kernel(index, where, *refs):
    parts, outs = refs[:4], refs[4:]
    pos = tuple(where[i] for i in range(4))
    for d, out in enumerate(outs):
        at = index(pos, d)
        total = parts[0][at].astype(F32)
        for part in parts[1:]:
            total = total + part[at].astype(F32)
        out[...] = total.astype(out.dtype)


def sum_and_cut(parts, where, index, shape, sends):
    size = int(np.prod(parts[0].shape))
    return pl.pallas_call(
        functools.partial(cut_kernel, index),
        out_shape=[jax.ShapeDtypeStruct(shape, F32)] + [jax.ShapeDtypeStruct(shape, BF16)] * sends,
        in_specs=[SMEM] + [VMEM] * 4,
        out_specs=[VMEM] * (sends + 1),
        cost_estimate=pl.CostEstimate(flops=size * 4, bytes_accessed=size * 12, transcendentals=0),
        compiler_params=pltpu.CompilerParams(vmem_limit_bytes=8 << 20),
    )(where, *parts)


def exchange(parts, axis):
    return [parts[0]] + [flip(parts[d], axis, d) for d in range(1, len(parts))]


def final_kernel(where, *refs):
    fx, fy, fz, out = refs[:4], refs[4:8], refs[8:10], refs[10]
    x, zl = where[0], where[2]
    quarter, half = ROWS_X // 4, ROWS_Z // 2
    for d in range(4):
        out[0, pl.ds(pl.multiple_of((x ^ d) * quarter, 16), quarter), :] = fx[d][...].astype(F32)
    total = fy[0][...]
    for part in fy[1:]:
        total = total + part[...].astype(F32)
    out[0, AT_Y : AT_Y + ROWS_Y, :] = total
    for d in range(2):
        out[0, pl.ds(pl.multiple_of(AT_Z + (zl ^ d) * half, 16), half), :] = fz[d][...].astype(F32)


def per_device(weight, activation, points):
    x, y, c = lax.axis_index("x"), lax.axis_index("y"), lax.axis_index("c")
    zl, zh = lax.axis_index("zl"), lax.axis_index("zh")
    where = jnp.stack([x, y, zl, zh, c]).astype(jnp.int32)
    factors = (points + 1).astype(F32) / 8
    view = weight.reshape(4, 2, 4, 2, 512, 128)

    pieces, parts, order = {}, {}, where
    for family in FAMILIES:
        sent, order = pack(family, view, activation, order)
        same = exchange(sent[:4], family)
        pieces[family] = same + [flip(sent[4 + d], family, d, 1) for d in range(4)]
    order, shared = order[:1], {}

    def share(family, order):
        xd, order = relay(family, pieces[family][:4], order)
        shared[family] = flip(xd, "c", 0, 1)
        return order

    for family in FAMILIES:
        order = share(family, order)
    for family in FAMILIES:
        parts[family], order = product(family, pieces[family], shared[family], where, factors, order)

    px = exchange(parts["x"], "z")
    py = exchange(parts["y"], "x")
    pz = exchange(parts["z"], "y")
    px = [p.reshape(4, 4, ROWS_X // 4, TOKENS) for p in px]
    py = [p.reshape(2, 2, ROWS_Y, TOKENS) for p in py]
    pz = [p.reshape(4, 2, ROWS_Z // 2, TOKENS) for p in pz]
    px = sum_and_cut(
        px, where, lambda pos, d: (slice(None), pos[1] ^ d), (4, ROWS_X // 4, TOKENS), 3)
    py = sum_and_cut(
        py, where, lambda pos, d: (pos[2] ^ (d & 1), pos[3] ^ (d >> 1)), (ROWS_Y, TOKENS), 3)
    pz = sum_and_cut(pz, where, lambda pos, d: (pos[0] ^ d,), (2, ROWS_Z // 2, TOKENS), 3)
    px = exchange(px, "y")
    py = exchange(py, "z")
    pz = exchange(pz, "x")
    px = sum_and_cut(px, where, lambda pos, d: (pos[0] ^ d,), (ROWS_X // 4, TOKENS), 3)
    pz = sum_and_cut(pz, where, lambda pos, d: (pos[2] ^ d,), (ROWS_Z // 2, TOKENS), 1)
    px = exchange(px, "x")
    pz = exchange(pz, "z")
    return pl.pallas_call(
        final_kernel,
        out_shape=jax.ShapeDtypeStruct((1, 512, TOKENS), F32),
        in_specs=[SMEM] + [VMEM] * 10,
        out_specs=VMEM,
        cost_estimate=pl.CostEstimate(flops=1 << 20, bytes_accessed=3 << 20, transcendentals=0),
        compiler_params=pltpu.CompilerParams(vmem_limit_bytes=8 << 20),
        name="final",
    )(where, *px, *py, *pz)


def solution(mesh):
    split = Mesh(mesh.devices.reshape(4, 2, 2, 4, 2), AXES)
    grp, mem = ("x", "zl"), ("zh", "y", "c")
    placed = (P(None, None, grp + mem), P(None, grp + mem, None), P())
    return jax.shard_map(per_device, mesh=split, in_specs=placed, out_specs=P(grp, mem, None), check_vma=False)
```

```python
import functools

import jax
import jax.numpy as jnp
import numpy as np
from jax import lax
from jax.experimental import pallas as pl
from jax.experimental.pallas import tpu as pltpu
from jax.sharding import Mesh
from jax.sharding import PartitionSpec as P


AXES = ("x", "zl", "zh", "y", "c")
SIZES = {"x": 4, "zl": 2, "zh": 2, "y": 4, "c": 2}
TOKENS = 512
FAMILIES = "zyx"
ROWS_X, ROWS_Y, ROWS_Z = 128, 192, 192
AT_Y, AT_Z = ROWS_X, ROWS_X + ROWS_Y
VMEM = pl.BlockSpec(memory_space=pltpu.VMEM)
SMEM = pl.BlockSpec(memory_space=pltpu.SMEM)
ANY = pl.BlockSpec(memory_space=pl.ANY)
HBM = pl.BlockSpec(memory_space=pltpu.HBM)
F32, BF16 = jnp.float32, jnp.bfloat16


def flip(value, axis, d, dc=0):
    over = [n for n in AXES if (n == "c" and dc) or (d and (n == axis or (axis == "z" and n in ("zl", "zh"))))]
    sizes = [SIZES[n] for n in over]
    pairs = []
    for i in range(int(np.prod(sizes))):
        at = dict(zip(over, (int(k) for k in np.unravel_index(i, sizes))))
        to = dict(at)
        if d and axis == "z":
            to["zl"] ^= d & 1
            to["zh"] ^= d >> 1
        elif d:
            to[axis] ^= d
        if dc:
            to["c"] ^= 1
        pairs.append((i, int(np.ravel_multi_index([to[n] for n in over], sizes))))
    return lax.ppermute(value, tuple(over), pairs)


def source_slices(family, w, where, d, dc):
    x, y, zl, zh, c = (where[i] for i in range(5))
    c = c ^ dc
    if family == "x":
        return w.at[:, :, :, c, pl.ds(pl.multiple_of((x ^ d) * (ROWS_X // 4), 16), ROWS_X // 4), :]
    if family == "y":
        return w.at[:, :, y ^ d, c, pl.ds(AT_Y, ROWS_Y), :]
    start = pl.multiple_of(AT_Z + (zl ^ (d & 1)) * (ROWS_Z // 2), 16)
    return w.at[:, zh ^ (d >> 1), :, c, pl.ds(start, ROWS_Z // 2), :]


PIECE = {
    "x": (4, 2, 4, ROWS_X // 4, 128),
    "y": (4, 2, ROWS_Y, 128),
    "z": (4, 4, ROWS_Z // 2, 128),
}
SOURCES = tuple((d, dc) for dc in (0, 1) for d in range(4))
CHUNK = 32
FEATURES = 2 * 4 * 128


def rows_of(family):
    return int(np.prod(PIECE[family][1:-1]))


def planes_of(family):
    return 4 + -(-FEATURES // rows_of(family))


def plane_at(shape, row):
    index, at = [], row
    for n in shape[::-1]:
        index.append(at % n)
        at //= n
    return (4 + at, *index[:0:-1], pl.ds(index[0], CHUNK))


def pack_kernel(family, where, w, act, *refs):
    outs, token, xstage, xin, sem, x_sem = refs[:8], refs[8], *refs[9:]
    read = pltpu.make_async_copy(act, xin, x_sem.at[0])
    read.start()
    copies = [
        pltpu.make_async_copy(
            source_slices(family, w, where, d, dc), out if dc else out.at[pl.ds(0, 4)], sem.at[i]
        )
        for i, ((d, dc), out) in enumerate(zip(SOURCES, outs))
    ]
    for copy in copies:
        copy.start()
    for i in range(5):
        token[i] = where[i]
    read.wait()
    for k in range(2):
        for ct in range(4):
            for r in range(0, 128, CHUNK):
                at = plane_at(PIECE[family][1:-1], (k * 4 + ct) * 128 + r)
                xstage[(at[0] - 4, *at[1:])] = xin[k, r : r + CHUNK, ct * 128 : (ct + 1) * 128]
    writes = [
        pltpu.make_async_copy(xstage, out.at[pl.ds(4, xstage.shape[0])], x_sem.at[i]) for i, out in enumerate(outs[:4])
    ]
    for write in writes:
        write.start()
    for copy in copies + writes:
        copy.wait()


def pack(family, weight, act, where):
    shape = PIECE[family]
    wide = (planes_of(family), *shape[1:])
    size = int(np.prod(shape)) * 2
    shapes = [jax.ShapeDtypeStruct(wide, BF16)] * 4 + [jax.ShapeDtypeStruct(shape, BF16)] * 4
    out = pl.pallas_call(
        functools.partial(pack_kernel, family),
        out_shape=shapes + [jax.ShapeDtypeStruct((5,), jnp.int32)],
        in_specs=[SMEM, HBM, HBM],
        out_specs=[ANY] * 8 + [SMEM],
        scratch_shapes=[
            pltpu.VMEM((wide[0] - 4, *shape[1:]), BF16),
            pltpu.VMEM(act.shape, BF16),
            pltpu.SemaphoreType.DMA((8,)),
            pltpu.SemaphoreType.DMA((4,)),
        ],
        cost_estimate=pl.CostEstimate(flops=0, bytes_accessed=16 * size, transcendentals=0),
        compiler_params=pltpu.CompilerParams(vmem_limit_bytes=4 << 20),
    )(where, weight, act)
    return out[:8], out[8]


def relay_kernel(order, *refs):
    pieces, out, token, sem = refs[:4], refs[4], refs[5], refs[6]
    copies = [pltpu.make_async_copy(p.at[pl.ds(4, out.shape[1])], out.at[i], sem.at[i]) for i, p in enumerate(pieces)]
    for copy in copies:
        copy.start()
    token[0] = order[0]
    for copy in copies:
        copy.wait()


def relay(family, pieces, order):
    shape = (4, planes_of(family) - 4, *PIECE[family][1:])
    return pl.pallas_call(
        relay_kernel,
        out_shape=[jax.ShapeDtypeStruct(shape, BF16), jax.ShapeDtypeStruct((1,), jnp.int32)],
        in_specs=[SMEM] + [ANY] * 4,
        out_specs=[VMEM, SMEM],
        scratch_shapes=[pltpu.SemaphoreType.DMA((4,))],
        cost_estimate=pl.CostEstimate(flops=0, bytes_accessed=4 << 20, transcendentals=0),
        compiler_params=pltpu.CompilerParams(vmem_limit_bytes=4 << 20),
    )(order, *pieces)


def plan_of(family, where):
    x, y, zl, zh = (where[i] for i in range(4))
    if family == "y":
        sends = [(d, gz, ((x ^ d) * 2 + gz)) for d in range(4) for gz in range(2)]
        return [(t * 96, 96, t * 96, sends) for t in range(4)]
    if family == "z":
        return [((y ^ d) * 96, 96, 0, [(d, g, g) for g in range(8)]) for d in range(4)]
    return [
        ((zh ^ e) * ROWS_X + t * 64, 64, t * 64,
         [(2 * e + f, gx, gx * 2 + (zl ^ f)) for f in range(2) for gx in range(4)])
        for e in range(2) for t in range(2)
    ]


OUT = {"x": (4, ROWS_X, TOKENS), "y": (2, 2 * ROWS_Y, TOKENS), "z": (8, ROWS_Z // 2, TOKENS)}
TILE = {"x": 64, "y": 96, "z": 96}


def product_kernel(family, where, factors, order, *refs):
    w, xd = refs[:8], refs[8]
    outs, token, xcat, prods = refs[9:13], refs[13], refs[14], refs[15:17]
    token[0] = order[0]
    rows, tile = rows_of(family), TILE[family]
    for s in range(8):
        for k in range(2):
            for ct in range(4):
                for r in range(0, 128, CHUNK):
                    at = plane_at((rows,), (k * 4 + ct) * 128 + r)
                    piece = w[s][at] if s < 4 else xd[(s - 4, at[0] - 4, *at[1:])]
                    xcat[s * 128 + r : s * 128 + r + CHUNK, k * TOKENS + ct * 128 : k * TOKENS + (ct + 1) * 128] = piece
    plan = plan_of(family, where)

    def multiply(start, prod):
        here = pl.ds(start if isinstance(start, int) else pl.multiple_of(start, 16), tile)
        left = [jnp.concatenate([w[s][j, here, :] for s in range(8)], axis=1) for j in range(4)]
        prod[...] = jnp.dot(jnp.concatenate(left, axis=0), xcat[...], preferred_element_type=F32)

    anchors = [factors[g] for g in range(8)] if family == "z" else None

    def combine(first, sends, prod):
        at = anchors or [factors[group] for _, _, group in sends]
        for r in range(0, tile, 8):
            for col in range(0, TOKENS, 256):
                terms = [
                    prod[(p % 4) * tile + r : (p % 4) * tile + r + 8, (p // 4) * TOKENS + col : (p // 4) * TOKENS + col + 256]
                    for p in range(8)
                ]
                for (d, slot, _), anchor in zip(sends, at):
                    total = terms[7]
                    for p in range(6, -1, -1):
                        total = total * anchor + terms[p]
                    outs[d][slot, first + r : first + r + 8, col : col + 256] = total.astype(BF16)

    multiply(plan[0][0], prods[0])
    for t in range(4):
        if t < 3:
            multiply(plan[t + 1][0], prods[(t + 1) % 2])
        combine(plan[t][2], plan[t][3], prods[t % 2])


def product(family, pieces, xd, where, factors, order):
    rows = rows_of(family)
    planes = planes_of(family)
    pieces = [p.reshape(-1, rows, 128) for p in pieces]
    xd = xd.reshape(4, planes - 4, rows, 128)
    flops = 2 * 4 * rows * 1024 * 1024
    out = pl.pallas_call(
        functools.partial(product_kernel, family),
        out_shape=[jax.ShapeDtypeStruct(OUT[family], BF16)] * 4 + [jax.ShapeDtypeStruct((1,), jnp.int32)],
        in_specs=[SMEM, SMEM, SMEM] + [VMEM] * 9,
        out_specs=[VMEM] * 4 + [SMEM],
        scratch_shapes=[pltpu.VMEM((1024, 1024), BF16)] + [pltpu.VMEM((4 * TILE[family], 1024), F32)] * 2,
        cost_estimate=pl.CostEstimate(flops=2 * flops, bytes_accessed=8 << 20, transcendentals=0),
        compiler_params=pltpu.CompilerParams(vmem_limit_bytes=22 << 20),
    )(where, factors, order, *pieces, xd)
    return out[:4], out[4]


def cut_kernel(index, where, *refs):
    parts, outs = refs[:4], refs[4:]
    pos = tuple(where[i] for i in range(4))
    for d, out in enumerate(outs):
        at = index(pos, d)
        total = parts[0][at].astype(F32)
        for part in parts[1:]:
            total = total + part[at].astype(F32)
        out[...] = total.astype(out.dtype)


def sum_and_cut(parts, where, index, shape, sends):
    size = int(np.prod(parts[0].shape))
    return pl.pallas_call(
        functools.partial(cut_kernel, index),
        out_shape=[jax.ShapeDtypeStruct(shape, F32)] + [jax.ShapeDtypeStruct(shape, BF16)] * sends,
        in_specs=[SMEM] + [VMEM] * 4,
        out_specs=[VMEM] * (sends + 1),
        cost_estimate=pl.CostEstimate(flops=size * 4, bytes_accessed=size * 12, transcendentals=0),
        compiler_params=pltpu.CompilerParams(vmem_limit_bytes=8 << 20),
    )(where, *parts)


def sum_kernel(*refs):
    total = refs[0][...].astype(F32)
    for part in refs[1:4]:
        total = total + part[...].astype(F32)
    refs[4][...] = total.astype(BF16)


def sum_all(parts):
    return pl.pallas_call(
        sum_kernel,
        out_shape=jax.ShapeDtypeStruct(parts[0].shape, BF16),
        in_specs=[VMEM] * 4,
        out_specs=VMEM,
        cost_estimate=pl.CostEstimate(flops=1 << 18, bytes_accessed=1 << 20, transcendentals=0),
        compiler_params=pltpu.CompilerParams(vmem_limit_bytes=8 << 20),
        name="sum2_x",
    )(*parts)


def exchange(parts, axis):
    return [parts[0]] + [flip(parts[d], axis, d) for d in range(1, len(parts))]


def final_kernel(where, *refs):
    fx, fy, fz, out = refs[0], refs[1:5], refs[5:7], refs[7]
    zl = where[2]
    quarter, half = ROWS_X // 4, ROWS_Z // 2
    for source in range(4):
        out[0, source * quarter : (source + 1) * quarter, :] = fx[source].astype(F32)
    total = fy[0][...]
    for part in fy[1:]:
        total = total + part[...].astype(F32)
    out[0, AT_Y : AT_Y + ROWS_Y, :] = total
    for d in range(2):
        out[0, pl.ds(pl.multiple_of(AT_Z + (zl ^ d) * half, 16), half), :] = fz[d][...].astype(F32)


def per_device(weight, activation, points):
    x, y, c = lax.axis_index("x"), lax.axis_index("y"), lax.axis_index("c")
    zl, zh = lax.axis_index("zl"), lax.axis_index("zh")
    where = jnp.stack([x, y, zl, zh, c]).astype(jnp.int32)
    factors = (points + 1).astype(F32) / 8
    view = weight.reshape(4, 2, 4, 2, 512, 128)

    pieces, parts, order = {}, {}, where
    for family in FAMILIES:
        sent, order = pack(family, view, activation, order)
        same = exchange(sent[:4], family)
        pieces[family] = same + [flip(sent[4 + d], family, d, 1) for d in range(4)]
    order, shared = order[:1], {}

    def share(family, order):
        xd, order = relay(family, pieces[family][:4], order)
        shared[family] = flip(xd, "c", 0, 1)
        return order

    for family in FAMILIES:
        order = share(family, order)
    for family in FAMILIES:
        parts[family], order = product(family, pieces[family], shared[family], where, factors, order)

    px = exchange(parts["x"], "z")
    py = exchange(parts["y"], "x")
    pz = exchange(parts["z"], "y")
    px = [p.reshape(4, 4, ROWS_X // 4, TOKENS) for p in px]
    py = [p.reshape(2, 2, ROWS_Y, TOKENS) for p in py]
    pz = [p.reshape(4, 2, ROWS_Z // 2, TOKENS) for p in pz]
    px = sum_and_cut(
        px, where, lambda pos, d: (slice(None), pos[1] ^ d), (4, ROWS_X // 4, TOKENS), 3)
    py = sum_and_cut(
        py, where, lambda pos, d: (pos[2] ^ (d & 1), pos[3] ^ (d >> 1)), (ROWS_Y, TOKENS), 3)
    pz = sum_and_cut(pz, where, lambda pos, d: (pos[0] ^ d,), (2, ROWS_Z // 2, TOKENS), 3)
    px = exchange(px, "y")
    py = exchange(py, "z")
    pz = exchange(pz, "x")
    px = sum_all(px)
    pz = sum_and_cut(pz, where, lambda pos, d: (pos[2] ^ d,), (ROWS_Z // 2, TOKENS), 1)
    px = lax.all_to_all(px, "x", split_axis=0, concat_axis=0, tiled=True)
    pz = exchange(pz, "z")
    return pl.pallas_call(
        final_kernel,
        out_shape=jax.ShapeDtypeStruct((1, 512, TOKENS), F32),
        in_specs=[SMEM] + [VMEM] * 7,
        out_specs=VMEM,
        cost_estimate=pl.CostEstimate(flops=1 << 20, bytes_accessed=3 << 20, transcendentals=0),
        compiler_params=pltpu.CompilerParams(vmem_limit_bytes=8 << 20),
        name="final",
    )(where, px, *py, *pz)


def solution(mesh):
    split = Mesh(mesh.devices.reshape(4, 2, 2, 4, 2), AXES)
    grp, mem = ("x", "zl"), ("zh", "y", "c")
    placed = (P(None, None, grp + mem), P(None, grp + mem, None), P())
    return jax.shard_map(per_device, mesh=split, in_specs=placed, out_specs=P(grp, mem, None), check_vma=False)
```

```python
import functools

import jax
import jax.numpy as jnp
import numpy as np
from jax import lax
from jax.experimental import pallas as pl
from jax.experimental.pallas import tpu as pltpu
from jax.sharding import Mesh
from jax.sharding import PartitionSpec as P


AXES = ("x", "zl", "zh", "y", "c")
SIZES = {"x": 4, "zl": 2, "zh": 2, "y": 4, "c": 2}
TOKENS = 512
FAMILIES = "yzx"
ROWS_X, ROWS_Y, ROWS_Z = 128, 192, 192
AT_Y, AT_Z = ROWS_X, ROWS_X + ROWS_Y
VMEM = pl.BlockSpec(memory_space=pltpu.VMEM)
SMEM = pl.BlockSpec(memory_space=pltpu.SMEM)
ANY = pl.BlockSpec(memory_space=pl.ANY)
HBM = pl.BlockSpec(memory_space=pltpu.HBM)
F32, BF16 = jnp.float32, jnp.bfloat16


def flip(value, axis, d, dc=0):
    over = [n for n in AXES if (n == "c" and dc) or (d and (n == axis or (axis == "z" and n in ("zl", "zh"))))]
    sizes = [SIZES[n] for n in over]
    pairs = []
    for i in range(int(np.prod(sizes))):
        at = dict(zip(over, (int(k) for k in np.unravel_index(i, sizes))))
        to = dict(at)
        if d and axis == "z":
            to["zl"] ^= d & 1
            to["zh"] ^= d >> 1
        elif d:
            to[axis] ^= d
        if dc:
            to["c"] ^= 1
        pairs.append((i, int(np.ravel_multi_index([to[n] for n in over], sizes))))
    return lax.ppermute(value, tuple(over), pairs)


def source_slices(family, w, where, d, dc):
    x, y, zl, zh, c = (where[i] for i in range(5))
    c = c ^ dc
    if family == "x":
        return w.at[:, :, :, c, pl.ds(pl.multiple_of((x ^ d) * (ROWS_X // 4), 16), ROWS_X // 4), :]
    if family == "y":
        return w.at[:, :, y ^ d, c, pl.ds(AT_Y, ROWS_Y), :]
    start = pl.multiple_of(AT_Z + (zl ^ (d & 1)) * (ROWS_Z // 2), 16)
    return w.at[:, zh ^ (d >> 1), :, c, pl.ds(start, ROWS_Z // 2), :]


PIECE = {
    "x": (4, 2, 4, ROWS_X // 4, 128),
    "y": (4, 2, ROWS_Y, 128),
    "z": (4, 4, ROWS_Z // 2, 128),
}
SOURCES = tuple((d, dc) for dc in (0, 1) for d in range(4))
CHUNK = 32
FEATURES = 2 * 4 * 128


def rows_of(family):
    return int(np.prod(PIECE[family][1:-1]))


def planes_of(family):
    return 4 + -(-FEATURES // rows_of(family))


def plane_at(shape, row):
    index, at = [], row
    for n in shape[::-1]:
        index.append(at % n)
        at //= n
    return (4 + at, *index[:0:-1], pl.ds(index[0], CHUNK))


def pack_kernel(family, where, w, act, *refs):
    outs, token, xstage, xin, sem, x_sem = refs[:8], refs[8], *refs[9:]
    read = pltpu.make_async_copy(act, xin, x_sem.at[0])
    read.start()
    copies = [
        pltpu.make_async_copy(
            source_slices(family, w, where, d, dc), out if dc else out.at[pl.ds(0, 4)], sem.at[i]
        )
        for i, ((d, dc), out) in enumerate(zip(SOURCES, outs))
    ]
    for copy in copies:
        copy.start()
    for i in range(5):
        token[i] = where[i]
    read.wait()
    for k in range(2):
        for ct in range(4):
            for r in range(0, 128, CHUNK):
                at = plane_at(PIECE[family][1:-1], (k * 4 + ct) * 128 + r)
                xstage[(at[0] - 4, *at[1:])] = xin[k, r : r + CHUNK, ct * 128 : (ct + 1) * 128]
    writes = [
        pltpu.make_async_copy(xstage, out.at[pl.ds(4, xstage.shape[0])], x_sem.at[i]) for i, out in enumerate(outs[:4])
    ]
    for write in writes:
        write.start()
    for copy in copies + writes:
        copy.wait()


def pack(family, weight, act, where):
    shape = PIECE[family]
    wide = (planes_of(family), *shape[1:])
    size = int(np.prod(shape)) * 2
    shapes = [jax.ShapeDtypeStruct(wide, BF16)] * 4 + [jax.ShapeDtypeStruct(shape, BF16)] * 4
    out = pl.pallas_call(
        functools.partial(pack_kernel, family),
        out_shape=shapes + [jax.ShapeDtypeStruct((5,), jnp.int32)],
        in_specs=[SMEM, HBM, HBM],
        out_specs=[ANY] * 8 + [SMEM],
        scratch_shapes=[
            pltpu.VMEM((wide[0] - 4, *shape[1:]), BF16),
            pltpu.VMEM(act.shape, BF16),
            pltpu.SemaphoreType.DMA((8,)),
            pltpu.SemaphoreType.DMA((4,)),
        ],
        cost_estimate=pl.CostEstimate(flops=0, bytes_accessed=16 * size, transcendentals=0),
        compiler_params=pltpu.CompilerParams(vmem_limit_bytes=4 << 20),
    )(where, weight, act)
    return out[:8], out[8]


def relay_kernel(order, *refs):
    pieces, out, token, sem = refs[:4], refs[4], refs[5], refs[6]
    copies = [pltpu.make_async_copy(p.at[pl.ds(4, out.shape[1])], out.at[i], sem.at[i]) for i, p in enumerate(pieces)]
    for copy in copies:
        copy.start()
    token[0] = order[0]
    for copy in copies:
        copy.wait()


def relay(family, pieces, order):
    shape = (4, planes_of(family) - 4, *PIECE[family][1:])
    return pl.pallas_call(
        relay_kernel,
        out_shape=[jax.ShapeDtypeStruct(shape, BF16), jax.ShapeDtypeStruct((1,), jnp.int32)],
        in_specs=[SMEM] + [ANY] * 4,
        out_specs=[VMEM, SMEM],
        scratch_shapes=[pltpu.SemaphoreType.DMA((4,))],
        cost_estimate=pl.CostEstimate(flops=0, bytes_accessed=4 << 20, transcendentals=0),
        compiler_params=pltpu.CompilerParams(vmem_limit_bytes=4 << 20),
    )(order, *pieces)


def plan_of(family, where):
    x, y, zl, zh = (where[i] for i in range(4))
    if family == "y":
        sends = [(d, gz, ((x ^ d) * 2 + gz)) for d in range(4) for gz in range(2)]
        return [(t * 96, 96, t * 96, sends) for t in range(4)]
    if family == "z":
        return [((y ^ d) * 96, 96, 0, [(d, g, g) for g in range(8)]) for d in range(4)]
    return [
        ((zh ^ e) * ROWS_X + t * 64, 64, t * 64,
         [(2 * e + f, gx, gx * 2 + (zl ^ f)) for f in range(2) for gx in range(4)])
        for e in range(2) for t in range(2)
    ]


OUT = {"x": (4, ROWS_X, TOKENS), "y": (2, 2 * ROWS_Y, TOKENS), "z": (8, ROWS_Z // 2, TOKENS)}
TILE = {"x": 64, "y": 96, "z": 96}


EARLY = FAMILIES[:2]


def fill(family, xcat, pieces, first):
    for s, (ref, *at) in enumerate(pieces):
        for k in range(2):
            for ct in range(4):
                for r in range(0, 128, CHUNK):
                    plane, rows = plane_at((rows_of(family),), (k * 4 + ct) * 128 + r)
                    xcat[s * 128 + r : s * 128 + r + CHUNK, k * TOKENS + ct * 128 : k * TOKENS + (ct + 1) * 128] = ref[
                        (*at, plane - 4 + (0 if at else first), rows)
                    ]


def times(family, w, start, xcat):
    tile = TILE[family]
    here = pl.ds(start if isinstance(start, int) else pl.multiple_of(start, 16), tile)
    left = [jnp.concatenate([ref[j, here, :] for ref in w], axis=1) for j in range(4)]
    return jnp.dot(jnp.concatenate(left, axis=0), xcat[...], preferred_element_type=F32)


def begin_kernel(family, where, order, *refs):
    w, out, token, xcat = refs[:4], refs[4], refs[5], refs[6]
    token[0] = order[0]
    fill(family, xcat, [(ref,) for ref in w], 4)
    for t, (start, *_) in enumerate(plan_of(family, where)):
        out[t] = times(family, w, start, xcat)


def begin(family, pieces, where, order):
    rows = rows_of(family)
    pieces = [p.reshape(-1, rows, 128) for p in pieces]
    return pl.pallas_call(
        functools.partial(begin_kernel, family),
        out_shape=[jax.ShapeDtypeStruct((4, 4 * TILE[family], 1024), F32), jax.ShapeDtypeStruct((1,), jnp.int32)],
        in_specs=[SMEM, SMEM] + [VMEM] * 4,
        out_specs=[VMEM, SMEM],
        scratch_shapes=[pltpu.VMEM((512, 1024), BF16)],
        cost_estimate=pl.CostEstimate(flops=4 * rows * 1024 * 1024, bytes_accessed=8 << 20, transcendentals=0),
        compiler_params=pltpu.CompilerParams(vmem_limit_bytes=11 << 20),
    )(where, order, *pieces)


def product_kernel(family, where, factors, order, *refs):
    early = family in EARLY
    n = 4 if early else 8
    w, xd, begun = refs[:n], refs[n], refs[n + 1] if early else None
    refs = refs[n + 1 + early :]
    outs, token, xcat, prods = refs[:4], refs[4], refs[5], refs[6:8]
    token[0] = order[0]
    tile = TILE[family]
    shared = [(xd, d) for d in range(4)]
    fill(family, xcat, shared if early else [(ref,) for ref in w[:4]] + shared, 4)
    plan = plan_of(family, where)
    anchors = [factors[g] for g in range(8)] if family == "z" else None

    def multiply(t, prod):
        total = times(family, w, plan[t][0], xcat)
        prod[...] = begun[t] + total if early else total

    def combine(first, sends, prod):
        at = anchors or [factors[group] for _, _, group in sends]
        for r in range(0, tile, 8):
            for col in range(0, TOKENS, 256):
                terms = [
                    prod[(p % 4) * tile + r : (p % 4) * tile + r + 8, (p // 4) * TOKENS + col : (p // 4) * TOKENS + col + 256]
                    for p in range(8)
                ]
                for (d, slot, _), anchor in zip(sends, at):
                    total = terms[7]
                    for p in range(6, -1, -1):
                        total = total * anchor + terms[p]
                    outs[d][slot, first + r : first + r + 8, col : col + 256] = total.astype(BF16)

    multiply(0, prods[0])
    for t in range(4):
        if t < 3:
            multiply(t + 1, prods[(t + 1) % 2])
        combine(plan[t][2], plan[t][3], prods[t % 2])


def product(family, pieces, xd, where, factors, order, begun):
    rows = rows_of(family)
    planes = planes_of(family)
    pieces = [p.reshape(-1, rows, 128) for p in (pieces[4:] if begun else pieces)]
    xd = xd.reshape(4, planes - 4, rows, 128)
    flops = 2 * 4 * rows * 1024 * 1024
    args = [*pieces, xd, *begun]
    out = pl.pallas_call(
        functools.partial(product_kernel, family),
        out_shape=[jax.ShapeDtypeStruct(OUT[family], BF16)] * 4 + [jax.ShapeDtypeStruct((1,), jnp.int32)],
        in_specs=[SMEM, SMEM, SMEM] + [VMEM] * len(args),
        out_specs=[VMEM] * 4 + [SMEM],
        scratch_shapes=[pltpu.VMEM((512 if begun else 1024, 1024), BF16)]
        + [pltpu.VMEM((4 * TILE[family], 1024), F32)] * 2,
        cost_estimate=pl.CostEstimate(flops=2 * flops, bytes_accessed=8 << 20, transcendentals=0),
        compiler_params=pltpu.CompilerParams(vmem_limit_bytes=12 << 20),
    )(where, factors, order, *args)
    return out[:4], out[4]


def cut_kernel(index, where, *refs):
    parts, outs = refs[:4], refs[4:]
    pos = tuple(where[i] for i in range(4))
    for d, out in enumerate(outs):
        at = index(pos, d)
        total = parts[0][at].astype(F32)
        for part in parts[1:]:
            total = total + part[at].astype(F32)
        out[...] = total.astype(out.dtype)


def sum_and_cut(parts, where, index, shape, sends):
    size = int(np.prod(parts[0].shape))
    return pl.pallas_call(
        functools.partial(cut_kernel, index),
        out_shape=[jax.ShapeDtypeStruct(shape, F32)] + [jax.ShapeDtypeStruct(shape, BF16)] * sends,
        in_specs=[SMEM] + [VMEM] * 4,
        out_specs=[VMEM] * (sends + 1),
        cost_estimate=pl.CostEstimate(flops=size * 4, bytes_accessed=size * 12, transcendentals=0),
        compiler_params=pltpu.CompilerParams(vmem_limit_bytes=8 << 20),
    )(where, *parts)


def exchange(parts, axis):
    return [parts[0]] + [flip(parts[d], axis, d) for d in range(1, len(parts))]


def close_kernel(where, *refs):
    fy, fz, out = refs[:4], refs[4:6], refs[6]
    zl, half = where[2], ROWS_Z // 2
    total = fy[0][...]
    for part in fy[1:]:
        total = total + part[...].astype(F32)
    out[0, AT_Y : AT_Y + ROWS_Y, :] = total
    for d in range(2):
        out[0, pl.ds(pl.multiple_of(AT_Z + (zl ^ d) * half, 16), half), :] = fz[d][...].astype(F32)


def final_kernel(where, *refs):
    fx, out, rows, sem = refs[:4], refs[5], refs[6], refs[7]
    x, quarter = where[0], ROWS_X // 4
    for d in range(4):
        rows[pl.ds(pl.multiple_of((x ^ d) * quarter, 16), quarter), :] = fx[d][...].astype(F32)
    copy = pltpu.make_async_copy(rows, out.at[0, pl.ds(0, ROWS_X)], sem.at[0])
    copy.start()
    copy.wait()


def per_device(weight, activation, points):
    x, y, c = lax.axis_index("x"), lax.axis_index("y"), lax.axis_index("c")
    zl, zh = lax.axis_index("zl"), lax.axis_index("zh")
    where = jnp.stack([x, y, zl, zh, c]).astype(jnp.int32)
    factors = (points + 1).astype(F32) / 8
    view = weight.reshape(4, 2, 4, 2, 512, 128)

    pieces, parts, order = {}, {}, where
    for family in FAMILIES:
        sent, order = pack(family, view, activation, order)
        same = exchange(sent[:4], family)
        pieces[family] = same + [flip(sent[4 + d], family, d, 1) for d in range(4)]
    order, shared = order[:1], {}

    def share(family, order):
        xd, order = relay(family, pieces[family][:4], order)
        shared[family] = flip(xd, "c", 0, 1)
        return order

    begun = {family: [] for family in FAMILIES}

    def early(family, order):
        product_so_far, order = begin(family, pieces[family][:4], where, order)
        begun[family] = [product_so_far]
        return order

    order = early(FAMILIES[0], share(FAMILIES[0], order))
    order = share(FAMILIES[2], share(FAMILIES[1], order))
    order = early(FAMILIES[1], order)
    for family in FAMILIES:
        parts[family], order = product(
            family, pieces[family], shared[family], where, factors, order, begun[family]
        )

    px = exchange(parts["x"], "z")
    py = exchange(parts["y"], "x")
    pz = exchange(parts["z"], "y")
    px = [p.reshape(4, 4, ROWS_X // 4, TOKENS) for p in px]
    py = [p.reshape(2, 2, ROWS_Y, TOKENS) for p in py]
    pz = [p.reshape(4, 2, ROWS_Z // 2, TOKENS) for p in pz]
    px = sum_and_cut(
        px, where, lambda pos, d: (slice(None), pos[1] ^ d), (4, ROWS_X // 4, TOKENS), 3)
    py = sum_and_cut(
        py, where, lambda pos, d: (pos[2] ^ (d & 1), pos[3] ^ (d >> 1)), (ROWS_Y, TOKENS), 3)
    pz = sum_and_cut(pz, where, lambda pos, d: (pos[0] ^ d,), (2, ROWS_Z // 2, TOKENS), 3)
    px = exchange(px, "y")
    py = exchange(py, "z")
    pz = exchange(pz, "x")
    px = sum_and_cut(px, where, lambda pos, d: (pos[0] ^ d,), (ROWS_X // 4, TOKENS), 3)
    pz = sum_and_cut(pz, where, lambda pos, d: (pos[2] ^ d,), (ROWS_Z // 2, TOKENS), 1)
    px = exchange(px, "x")
    pz = exchange(pz, "z")
    out = pl.pallas_call(
        close_kernel,
        out_shape=jax.ShapeDtypeStruct((1, 512, TOKENS), F32),
        in_specs=[SMEM] + [VMEM] * 6,
        out_specs=VMEM,
        cost_estimate=pl.CostEstimate(flops=1 << 20, bytes_accessed=3 << 20, transcendentals=0),
        compiler_params=pltpu.CompilerParams(vmem_limit_bytes=8 << 20),
        name="close",
    )(where, *py, *pz)
    return pl.pallas_call(
        final_kernel,
        out_shape=jax.ShapeDtypeStruct((1, 512, TOKENS), F32),
        in_specs=[SMEM] + [VMEM] * 4 + [HBM],
        out_specs=HBM,
        input_output_aliases={5: 0},
        scratch_shapes=[pltpu.VMEM((ROWS_X, TOKENS), F32), pltpu.SemaphoreType.DMA((1,))],
        cost_estimate=pl.CostEstimate(flops=1 << 16, bytes_accessed=1 << 19, transcendentals=0),
        compiler_params=pltpu.CompilerParams(vmem_limit_bytes=4 << 20),
        name="final",
    )(where, *px, out)


def solution(mesh):
    split = Mesh(mesh.devices.reshape(4, 2, 2, 4, 2), AXES)
    grp, mem = ("x", "zl"), ("zh", "y", "c")
    placed = (P(None, None, grp + mem), P(None, grp + mem, None), P())
    return jax.shard_map(per_device, mesh=split, in_specs=placed, out_specs=P(grp, mem, None), check_vma=False)
```

```python
import functools

import jax
import jax.numpy as jnp
import numpy as np
from jax import lax
from jax.experimental import pallas as pl
from jax.experimental.pallas import tpu as pltpu
from jax.sharding import Mesh
from jax.sharding import PartitionSpec as P


AXES = ("x", "zl", "zh", "y", "c")
SIZES = {"x": 4, "zl": 2, "zh": 2, "y": 4, "c": 2}
TOKENS = 512
FAMILIES = "yzx"
ROWS_X, ROWS_Y, ROWS_Z = 128, 192, 192
AT_Y, AT_Z = ROWS_X, ROWS_X + ROWS_Y
VMEM = pl.BlockSpec(memory_space=pltpu.VMEM)
SMEM = pl.BlockSpec(memory_space=pltpu.SMEM)
ANY = pl.BlockSpec(memory_space=pl.ANY)
HBM = pl.BlockSpec(memory_space=pltpu.HBM)
F32, BF16 = jnp.float32, jnp.bfloat16


def flip(value, axis, d, dc=0):
    over = [n for n in AXES if (n == "c" and dc) or (d and (n == axis or (axis == "z" and n in ("zl", "zh"))))]
    sizes = [SIZES[n] for n in over]
    pairs = []
    for i in range(int(np.prod(sizes))):
        at = dict(zip(over, (int(k) for k in np.unravel_index(i, sizes))))
        to = dict(at)
        if d and axis == "z":
            to["zl"] ^= d & 1
            to["zh"] ^= d >> 1
        elif d:
            to[axis] ^= d
        if dc:
            to["c"] ^= 1
        pairs.append((i, int(np.ravel_multi_index([to[n] for n in over], sizes))))
    return lax.ppermute(value, tuple(over), pairs)


def source_slices(family, w, where, d, dc):
    x, y, zl, zh, c = (where[i] for i in range(5))
    c = c ^ dc
    if family == "x":
        return w.at[:, :, :, c, pl.ds(pl.multiple_of((x ^ d) * (ROWS_X // 4), 16), ROWS_X // 4), :]
    if family == "y":
        return w.at[:, :, y ^ d, c, pl.ds(AT_Y, ROWS_Y), :]
    start = pl.multiple_of(AT_Z + (zl ^ (d & 1)) * (ROWS_Z // 2), 16)
    return w.at[:, zh ^ (d >> 1), :, c, pl.ds(start, ROWS_Z // 2), :]


PIECE = {
    "x": (4, 2, 4, ROWS_X // 4, 128),
    "y": (4, 2, ROWS_Y, 128),
    "z": (4, 4, ROWS_Z // 2, 128),
}
SOURCES = tuple((d, dc) for dc in (0, 1) for d in range(4))
CHUNK = 32
FEATURES = 2 * 4 * 128


def rows_of(family):
    return int(np.prod(PIECE[family][1:-1]))


def planes_of(family):
    return 4 + -(-FEATURES // rows_of(family))


def plane_at(shape, row):
    index, at = [], row
    for n in shape[::-1]:
        index.append(at % n)
        at //= n
    return (4 + at, *index[:0:-1], pl.ds(index[0], CHUNK))


def pack_kernel(family, where, w, act, *refs):
    outs, token, xstage, xin, sem, x_sem = refs[:8], refs[8], *refs[9:]
    read = pltpu.make_async_copy(act, xin, x_sem.at[0])
    read.start()
    copies = [
        pltpu.make_async_copy(
            source_slices(family, w, where, d, dc), out if dc else out.at[pl.ds(0, 4)], sem.at[i]
        )
        for i, ((d, dc), out) in enumerate(zip(SOURCES, outs))
    ]
    for copy in copies:
        copy.start()
    for i in range(5):
        token[i] = where[i]
    read.wait()
    for k in range(2):
        for ct in range(4):
            for r in range(0, 128, CHUNK):
                at = plane_at(PIECE[family][1:-1], (k * 4 + ct) * 128 + r)
                xstage[(at[0] - 4, *at[1:])] = xin[k, r : r + CHUNK, ct * 128 : (ct + 1) * 128]
    writes = [
        pltpu.make_async_copy(xstage, out.at[pl.ds(4, xstage.shape[0])], x_sem.at[i]) for i, out in enumerate(outs[:4])
    ]
    for write in writes:
        write.start()
    for copy in copies + writes:
        copy.wait()


def pack(family, weight, act, where):
    shape = PIECE[family]
    wide = (planes_of(family), *shape[1:])
    size = int(np.prod(shape)) * 2
    shapes = [jax.ShapeDtypeStruct(wide, BF16)] * 4 + [jax.ShapeDtypeStruct(shape, BF16)] * 4
    out = pl.pallas_call(
        functools.partial(pack_kernel, family),
        out_shape=shapes + [jax.ShapeDtypeStruct((5,), jnp.int32)],
        in_specs=[SMEM, HBM, HBM],
        out_specs=[ANY] * 8 + [SMEM],
        scratch_shapes=[
            pltpu.VMEM((wide[0] - 4, *shape[1:]), BF16),
            pltpu.VMEM(act.shape, BF16),
            pltpu.SemaphoreType.DMA((8,)),
            pltpu.SemaphoreType.DMA((4,)),
        ],
        cost_estimate=pl.CostEstimate(flops=0, bytes_accessed=16 * size, transcendentals=0),
        compiler_params=pltpu.CompilerParams(vmem_limit_bytes=4 << 20),
    )(where, weight, act)
    return out[:8], out[8]


def relay_kernel(order, *refs):
    pieces, out, token, sem = refs[:4], refs[4], refs[5], refs[6]
    copies = [pltpu.make_async_copy(p.at[pl.ds(4, out.shape[1])], out.at[i], sem.at[i]) for i, p in enumerate(pieces)]
    for copy in copies:
        copy.start()
    token[0] = order[0]
    for copy in copies:
        copy.wait()


def relay(family, pieces, order):
    shape = (4, planes_of(family) - 4, *PIECE[family][1:])
    return pl.pallas_call(
        relay_kernel,
        out_shape=[jax.ShapeDtypeStruct(shape, BF16), jax.ShapeDtypeStruct((1,), jnp.int32)],
        in_specs=[SMEM] + [ANY] * 4,
        out_specs=[VMEM, SMEM],
        scratch_shapes=[pltpu.SemaphoreType.DMA((4,))],
        cost_estimate=pl.CostEstimate(flops=0, bytes_accessed=4 << 20, transcendentals=0),
        compiler_params=pltpu.CompilerParams(vmem_limit_bytes=4 << 20),
    )(order, *pieces)


def plan_of(family, where):
    x, y, zl, zh = (where[i] for i in range(4))
    if family == "y":
        sends = [(d, gz, ((x ^ d) * 2 + gz)) for d in range(4) for gz in range(2)]
        return [(t * 96, 96, t * 96, sends) for t in range(4)]
    if family == "z":
        return [((y ^ d) * 96, 96, 0, [(d, g, g) for g in range(8)]) for d in range(4)]
    return [
        ((zh ^ e) * ROWS_X + t * 64, 64, t * 64,
         [(2 * e + f, gx, gx * 2 + (zl ^ f)) for f in range(2) for gx in range(4)])
        for e in range(2) for t in range(2)
    ]


OUT = {"x": (4, ROWS_X, TOKENS), "y": (2, 2 * ROWS_Y, TOKENS), "z": (8, ROWS_Z // 2, TOKENS)}
TILE = {"x": 64, "y": 96, "z": 96}


EARLY = FAMILIES[:2]


def fill(family, xcat, pieces, first):
    for s, (ref, *at) in enumerate(pieces):
        for k in range(2):
            for ct in range(4):
                for r in range(0, 128, CHUNK):
                    plane, rows = plane_at((rows_of(family),), (k * 4 + ct) * 128 + r)
                    xcat[s * 128 + r : s * 128 + r + CHUNK, k * TOKENS + ct * 128 : k * TOKENS + (ct + 1) * 128] = ref[
                        (*at, plane - 4 + (0 if at else first), rows)
                    ]


def times(family, w, start, xcat):
    tile = TILE[family]
    here = pl.ds(start if isinstance(start, int) else pl.multiple_of(start, 16), tile)
    left = [jnp.concatenate([ref[j, here, :] for ref in w], axis=1) for j in range(4)]
    return jnp.dot(jnp.concatenate(left, axis=0), xcat[...], preferred_element_type=F32)


def begin_kernel(family, where, order, *refs):
    w, out, token, xcat = refs[:4], refs[4], refs[5], refs[6]
    token[0] = order[0]
    fill(family, xcat, [(ref,) for ref in w], 4)
    for t, (start, *_) in enumerate(plan_of(family, where)):
        out[t] = times(family, w, start, xcat)


def begin(family, pieces, where, order):
    rows = rows_of(family)
    pieces = [p.reshape(-1, rows, 128) for p in pieces]
    return pl.pallas_call(
        functools.partial(begin_kernel, family),
        out_shape=[jax.ShapeDtypeStruct((4, 4 * TILE[family], 1024), F32), jax.ShapeDtypeStruct((1,), jnp.int32)],
        in_specs=[SMEM, SMEM] + [VMEM] * 4,
        out_specs=[VMEM, SMEM],
        scratch_shapes=[pltpu.VMEM((512, 1024), BF16)],
        cost_estimate=pl.CostEstimate(flops=4 * rows * 1024 * 1024, bytes_accessed=8 << 20, transcendentals=0),
        compiler_params=pltpu.CompilerParams(vmem_limit_bytes=11 << 20),
    )(where, order, *pieces)


def product_kernel(family, where, factors, order, *refs):
    early = family in EARLY
    n = 4 if early else 8
    w, xd, begun = refs[:n], refs[n], refs[n + 1] if early else None
    refs = refs[n + 1 + early :]
    outs, token, xcat, prods = refs[:4], refs[4], refs[5], refs[6:8]
    token[0] = order[0]
    tile = TILE[family]
    shared = [(xd, d) for d in range(4)]
    fill(family, xcat, shared if early else [(ref,) for ref in w[:4]] + shared, 4)
    plan = plan_of(family, where)
    anchors = [factors[g] for g in range(8)] if family == "z" else None

    def multiply(t, prod):
        total = times(family, w, plan[t][0], xcat)
        prod[...] = begun[t] + total if early else total

    def combine(first, sends, prod):
        at = anchors or [factors[group] for _, _, group in sends]
        for r in range(0, tile, 8):
            for col in range(0, TOKENS, 256):
                terms = [
                    prod[(p % 4) * tile + r : (p % 4) * tile + r + 8, (p // 4) * TOKENS + col : (p // 4) * TOKENS + col + 256]
                    for p in range(8)
                ]
                for (d, slot, _), anchor in zip(sends, at):
                    total = terms[7]
                    for p in range(6, -1, -1):
                        total = total * anchor + terms[p]
                    outs[d][slot, first + r : first + r + 8, col : col + 256] = total.astype(BF16)

    multiply(0, prods[0])
    for t in range(4):
        if t < 3:
            multiply(t + 1, prods[(t + 1) % 2])
        combine(plan[t][2], plan[t][3], prods[t % 2])


def product(family, pieces, xd, where, factors, order, begun):
    rows = rows_of(family)
    planes = planes_of(family)
    pieces = [p.reshape(-1, rows, 128) for p in (pieces[4:] if begun else pieces)]
    xd = xd.reshape(4, planes - 4, rows, 128)
    flops = 2 * 4 * rows * 1024 * 1024
    args = [*pieces, xd, *begun]
    out = pl.pallas_call(
        functools.partial(product_kernel, family),
        out_shape=[jax.ShapeDtypeStruct(OUT[family], BF16)] * 4 + [jax.ShapeDtypeStruct((1,), jnp.int32)],
        in_specs=[SMEM, SMEM, SMEM] + [VMEM] * len(args),
        out_specs=[VMEM] * 4 + [SMEM],
        scratch_shapes=[pltpu.VMEM((512 if begun else 1024, 1024), BF16)]
        + [pltpu.VMEM((4 * TILE[family], 1024), F32)] * 2,
        cost_estimate=pl.CostEstimate(flops=2 * flops, bytes_accessed=8 << 20, transcendentals=0),
        compiler_params=pltpu.CompilerParams(vmem_limit_bytes=12 << 20),
    )(where, factors, order, *args)
    return out[:4], out[4]


def cut_kernel(index, where, *refs):
    parts, outs = refs[:4], refs[4:]
    pos = tuple(where[i] for i in range(4))
    for d, out in enumerate(outs):
        at = index(pos, d)
        total = parts[0][at].astype(F32)
        for part in parts[1:]:
            total = total + part[at].astype(F32)
        out[...] = total.astype(out.dtype)


def sum_and_cut(parts, where, index, shape, sends):
    size = int(np.prod(parts[0].shape))
    return pl.pallas_call(
        functools.partial(cut_kernel, index),
        out_shape=[jax.ShapeDtypeStruct(shape, F32)] + [jax.ShapeDtypeStruct(shape, BF16)] * sends,
        in_specs=[SMEM] + [VMEM] * 4,
        out_specs=[VMEM] * (sends + 1),
        cost_estimate=pl.CostEstimate(flops=size * 4, bytes_accessed=size * 12, transcendentals=0),
        compiler_params=pltpu.CompilerParams(vmem_limit_bytes=8 << 20),
    )(where, *parts)


def exchange(parts, axis):
    arrived = {0: parts[0]}
    for d in (2, 1, 3):
        if d < len(parts):
            arrived[d] = flip(parts[d], axis, d)
    return [arrived[d] for d in range(len(parts))]


def close_kernel(where, *refs):
    fy, fz, out = refs[:4], refs[4:6], refs[6]
    zl, half = where[2], ROWS_Z // 2
    total = fy[0][...]
    for part in fy[1:]:
        total = total + part[...].astype(F32)
    out[0, AT_Y : AT_Y + ROWS_Y, :] = total
    for d in range(2):
        out[0, pl.ds(pl.multiple_of(AT_Z + (zl ^ d) * half, 16), half), :] = fz[d][...].astype(F32)


def final_kernel(where, *refs):
    fx, out, rows, sem = refs[:4], refs[5], refs[6], refs[7]
    x, quarter = where[0], ROWS_X // 4
    for d in range(4):
        rows[pl.ds(pl.multiple_of((x ^ d) * quarter, 16), quarter), :] = fx[d][...].astype(F32)
    copy = pltpu.make_async_copy(rows, out.at[0, pl.ds(0, ROWS_X)], sem.at[0])
    copy.start()
    copy.wait()


def per_device(weight, activation, points):
    x, y, c = lax.axis_index("x"), lax.axis_index("y"), lax.axis_index("c")
    zl, zh = lax.axis_index("zl"), lax.axis_index("zh")
    where = jnp.stack([x, y, zl, zh, c]).astype(jnp.int32)
    factors = (points + 1).astype(F32) / 8
    view = weight.reshape(4, 2, 4, 2, 512, 128)

    pieces, parts, order = {}, {}, where
    for family in FAMILIES:
        sent, order = pack(family, view, activation, order)
        same = exchange(sent[:4], family)
        cross = {d: flip(sent[4 + d], family, d, 1) for d in (2, 1, 3, 0)}
        pieces[family] = same + [cross[d] for d in range(4)]
    order, shared = order[:1], {}

    def share(family, order):
        xd, order = relay(family, pieces[family][:4], order)
        shared[family] = flip(xd, "c", 0, 1)
        return order

    begun = {family: [] for family in FAMILIES}

    def early(family, order):
        product_so_far, order = begin(family, pieces[family][:4], where, order)
        begun[family] = [product_so_far]
        return order

    order = early(FAMILIES[0], share(FAMILIES[0], order))
    order = early(FAMILIES[1], share(FAMILIES[1], order))
    for family in FAMILIES:
        if family == FAMILIES[2]:
            order = share(family, order)
        parts[family], order = product(
            family, pieces[family], shared[family], where, factors, order, begun[family]
        )

    px = exchange(parts["x"], "z")
    py = exchange(parts["y"], "x")
    pz = exchange(parts["z"], "y")
    px = [p.reshape(4, 4, ROWS_X // 4, TOKENS) for p in px]
    py = [p.reshape(2, 2, ROWS_Y, TOKENS) for p in py]
    pz = [p.reshape(4, 2, ROWS_Z // 2, TOKENS) for p in pz]
    px = sum_and_cut(
        px, where, lambda pos, d: (slice(None), pos[1] ^ d), (4, ROWS_X // 4, TOKENS), 3)
    py = sum_and_cut(
        py, where, lambda pos, d: (pos[2] ^ (d & 1), pos[3] ^ (d >> 1)), (ROWS_Y, TOKENS), 3)
    pz = sum_and_cut(pz, where, lambda pos, d: (pos[0] ^ d,), (2, ROWS_Z // 2, TOKENS), 3)
    px = exchange(px, "y")
    py = exchange(py, "z")
    pz = exchange(pz, "x")
    px = sum_and_cut(px, where, lambda pos, d: (pos[0] ^ d,), (ROWS_X // 4, TOKENS), 3)
    pz = sum_and_cut(pz, where, lambda pos, d: (pos[2] ^ d,), (ROWS_Z // 2, TOKENS), 1)
    px = exchange(px, "x")
    pz = exchange(pz, "z")
    out = pl.pallas_call(
        close_kernel,
        out_shape=jax.ShapeDtypeStruct((1, 512, TOKENS), F32),
        in_specs=[SMEM] + [VMEM] * 6,
        out_specs=VMEM,
        cost_estimate=pl.CostEstimate(flops=1 << 20, bytes_accessed=3 << 20, transcendentals=0),
        compiler_params=pltpu.CompilerParams(vmem_limit_bytes=8 << 20),
        name="close",
    )(where, *py, *pz)
    return pl.pallas_call(
        final_kernel,
        out_shape=jax.ShapeDtypeStruct((1, 512, TOKENS), F32),
        in_specs=[SMEM] + [VMEM] * 4 + [HBM],
        out_specs=HBM,
        input_output_aliases={5: 0},
        scratch_shapes=[pltpu.VMEM((ROWS_X, TOKENS), F32), pltpu.SemaphoreType.DMA((1,))],
        cost_estimate=pl.CostEstimate(flops=1 << 16, bytes_accessed=1 << 19, transcendentals=0),
        compiler_params=pltpu.CompilerParams(vmem_limit_bytes=4 << 20),
        name="final",
    )(where, *px, out)


def solution(mesh):
    split = Mesh(mesh.devices.reshape(4, 2, 2, 4, 2), AXES)
    grp, mem = ("x", "zl"), ("zh", "y", "c")
    placed = (P(None, None, grp + mem), P(None, grp + mem, None), P())
    return jax.shard_map(per_device, mesh=split, in_specs=placed, out_specs=P(grp, mem, None), check_vma=False)
```

```python
import functools

import jax
import jax.numpy as jnp
import numpy as np
from jax import lax
from jax.experimental import pallas as pl
from jax.experimental.pallas import tpu as pltpu
from jax.sharding import Mesh
from jax.sharding import PartitionSpec as P


AXES = ("x", "zl", "zh", "y", "c")
SIZES = {"x": 4, "zl": 2, "zh": 2, "y": 4, "c": 2}
TOKENS = 512
FAMILIES = "yzx"
ROWS_X, ROWS_Y, ROWS_Z = 128, 192, 192
AT_Y, AT_Z = ROWS_X, ROWS_X + ROWS_Y
VMEM = pl.BlockSpec(memory_space=pltpu.VMEM)
SMEM = pl.BlockSpec(memory_space=pltpu.SMEM)
ANY = pl.BlockSpec(memory_space=pl.ANY)
HBM = pl.BlockSpec(memory_space=pltpu.HBM)
F32, BF16 = jnp.float32, jnp.bfloat16


def flip(value, axis, d, dc=0):
    over = [n for n in AXES if (n == "c" and dc) or (d and (n == axis or (axis == "z" and n in ("zl", "zh"))))]
    sizes = [SIZES[n] for n in over]
    pairs = []
    for i in range(int(np.prod(sizes))):
        at = dict(zip(over, (int(k) for k in np.unravel_index(i, sizes))))
        to = dict(at)
        if d and axis == "z":
            to["zl"] ^= d & 1
            to["zh"] ^= d >> 1
        elif d:
            to[axis] ^= d
        if dc:
            to["c"] ^= 1
        pairs.append((i, int(np.ravel_multi_index([to[n] for n in over], sizes))))
    return lax.ppermute(value, tuple(over), pairs)


def source_slices(family, w, where, d, dc):
    x, y, zl, zh, c = (where[i] for i in range(5))
    c = c ^ dc
    if family == "x":
        return w.at[:, :, :, c, pl.ds(pl.multiple_of((x ^ d) * (ROWS_X // 4), 16), ROWS_X // 4), :]
    if family == "y":
        return w.at[:, :, y ^ d, c, pl.ds(AT_Y, ROWS_Y), :]
    start = pl.multiple_of(AT_Z + (zl ^ (d & 1)) * (ROWS_Z // 2), 16)
    return w.at[:, zh ^ (d >> 1), :, c, pl.ds(start, ROWS_Z // 2), :]


PIECE = {
    "x": (4, 2, 4, ROWS_X // 4, 128),
    "y": (4, 2, ROWS_Y, 128),
    "z": (4, 4, ROWS_Z // 2, 128),
}
SOURCES = tuple((d, dc) for dc in (0, 1) for d in range(4))
CHUNK = 32
FEATURES = 2 * 4 * 128


def rows_of(family):
    return int(np.prod(PIECE[family][1:-1]))


def planes_of(family):
    return 4 + -(-FEATURES // rows_of(family))


def plane_at(shape, row):
    index, at = [], row
    for n in shape[::-1]:
        index.append(at % n)
        at //= n
    return (4 + at, *index[:0:-1], pl.ds(index[0], CHUNK))


def pack_kernel(family, where, w, act, *refs):
    outs, token, xstage, xin, sem, x_sem = refs[:8], refs[8], *refs[9:]
    read = pltpu.make_async_copy(act, xin, x_sem.at[0])
    read.start()
    copies = [
        pltpu.make_async_copy(
            source_slices(family, w, where, d, dc), out if dc else out.at[pl.ds(0, 4)], sem.at[i]
        )
        for i, ((d, dc), out) in enumerate(zip(SOURCES, outs))
    ]
    for copy in copies:
        copy.start()
    for i in range(5):
        token[i] = where[i]
    read.wait()
    for k in range(2):
        for ct in range(4):
            for r in range(0, 128, CHUNK):
                at = plane_at(PIECE[family][1:-1], (k * 4 + ct) * 128 + r)
                xstage[(at[0] - 4, *at[1:])] = xin[k, r : r + CHUNK, ct * 128 : (ct + 1) * 128]
    writes = [
        pltpu.make_async_copy(xstage, out.at[pl.ds(4, xstage.shape[0])], x_sem.at[i]) for i, out in enumerate(outs[:4])
    ]
    for write in writes:
        write.start()
    for copy in copies + writes:
        copy.wait()


def pack(family, weight, act, where):
    shape = PIECE[family]
    wide = (planes_of(family), *shape[1:])
    size = int(np.prod(shape)) * 2
    shapes = [jax.ShapeDtypeStruct(wide, BF16)] * 4 + [jax.ShapeDtypeStruct(shape, BF16)] * 4
    out = pl.pallas_call(
        functools.partial(pack_kernel, family),
        out_shape=shapes + [jax.ShapeDtypeStruct((5,), jnp.int32)],
        in_specs=[SMEM, HBM, HBM],
        out_specs=[ANY] * 8 + [SMEM],
        scratch_shapes=[
            pltpu.VMEM((wide[0] - 4, *shape[1:]), BF16),
            pltpu.VMEM(act.shape, BF16),
            pltpu.SemaphoreType.DMA((8,)),
            pltpu.SemaphoreType.DMA((4,)),
        ],
        cost_estimate=pl.CostEstimate(flops=0, bytes_accessed=16 * size, transcendentals=0),
        compiler_params=pltpu.CompilerParams(vmem_limit_bytes=4 << 20),
    )(where, weight, act)
    return out[:8], out[8]


def relay_kernel(order, *refs):
    pieces, out, token, sem = refs[:4], refs[4], refs[5], refs[6]
    copies = [pltpu.make_async_copy(p.at[pl.ds(4, out.shape[1])], out.at[i], sem.at[i]) for i, p in enumerate(pieces)]
    for copy in copies:
        copy.start()
    token[0] = order[0]
    for copy in copies:
        copy.wait()


def relay(family, pieces, order):
    shape = (4, planes_of(family) - 4, *PIECE[family][1:])
    return pl.pallas_call(
        relay_kernel,
        out_shape=[jax.ShapeDtypeStruct(shape, BF16), jax.ShapeDtypeStruct((1,), jnp.int32)],
        in_specs=[SMEM] + [ANY] * 4,
        out_specs=[VMEM, SMEM],
        scratch_shapes=[pltpu.SemaphoreType.DMA((4,))],
        cost_estimate=pl.CostEstimate(flops=0, bytes_accessed=4 << 20, transcendentals=0),
        compiler_params=pltpu.CompilerParams(vmem_limit_bytes=4 << 20),
    )(order, *pieces)


def plan_of(family, where):
    x, y, zl, zh = (where[i] for i in range(4))
    if family == "y":
        sends = [(d, gz, ((x ^ d) * 2 + gz)) for d in range(4) for gz in range(2)]
        return [(t * 96, 96, t * 96, sends) for t in range(4)]
    if family == "z":
        return [((y ^ d) * 96, 96, 0, [(d, g, g) for g in range(8)]) for d in range(4)]
    return [
        ((zh ^ e) * ROWS_X + t * 64, 64, t * 64,
         [(2 * e + f, gx, gx * 2 + (zl ^ f)) for f in range(2) for gx in range(4)])
        for e in range(2) for t in range(2)
    ]


OUT = {"x": (4, ROWS_X, TOKENS), "y": (2, 2 * ROWS_Y, TOKENS), "z": (8, ROWS_Z // 2, TOKENS)}
TILE = {"x": 64, "y": 96, "z": 96}


EARLY = FAMILIES[:2]


def fill(family, xcat, pieces, first):
    for s, (ref, *at) in enumerate(pieces):
        for k in range(2):
            for ct in range(4):
                for r in range(0, 128, CHUNK):
                    plane, rows = plane_at((rows_of(family),), (k * 4 + ct) * 128 + r)
                    xcat[s * 128 + r : s * 128 + r + CHUNK, k * TOKENS + ct * 128 : k * TOKENS + (ct + 1) * 128] = ref[
                        (*at, plane - 4 + (0 if at else first), rows)
                    ]


def times(family, w, start, xcat):
    tile = TILE[family]
    here = pl.ds(start if isinstance(start, int) else pl.multiple_of(start, 16), tile)
    left = [jnp.concatenate([ref[j, here, :] for ref in w], axis=1) for j in range(4)]
    return jnp.dot(jnp.concatenate(left, axis=0), xcat[...], preferred_element_type=F32)


def begin_kernel(family, where, order, *refs):
    w, out, token, xcat = refs[:4], refs[4], refs[5], refs[6]
    token[0] = order[0]
    fill(family, xcat, [(ref,) for ref in w], 4)
    for t, (start, *_) in enumerate(plan_of(family, where)):
        out[t] = times(family, w, start, xcat)


def begin(family, pieces, where, order):
    rows = rows_of(family)
    pieces = [p.reshape(-1, rows, 128) for p in pieces]
    return pl.pallas_call(
        functools.partial(begin_kernel, family),
        out_shape=[jax.ShapeDtypeStruct((4, 4 * TILE[family], 1024), F32), jax.ShapeDtypeStruct((1,), jnp.int32)],
        in_specs=[SMEM, SMEM] + [VMEM] * 4,
        out_specs=[VMEM, SMEM],
        scratch_shapes=[pltpu.VMEM((512, 1024), BF16)],
        cost_estimate=pl.CostEstimate(flops=4 * rows * 1024 * 1024, bytes_accessed=8 << 20, transcendentals=0),
        compiler_params=pltpu.CompilerParams(vmem_limit_bytes=11 << 20),
    )(where, order, *pieces)


def product_kernel(family, where, factors, order, *refs):
    early = family in EARLY
    n = 4 if early else 8
    w, xd, begun = refs[:n], refs[n], refs[n + 1] if early else None
    refs = refs[n + 1 + early :]
    outs, token, xcat, prods = refs[:4], refs[4], refs[5], refs[6:8]
    token[0] = order[0]
    tile = TILE[family]
    shared = [(xd, d) for d in range(4)]
    fill(family, xcat, shared if early else [(ref,) for ref in w[:4]] + shared, 4)
    plan = plan_of(family, where)
    anchors = [factors[g] for g in range(8)] if family == "z" else None

    def multiply(t, prod):
        total = times(family, w, plan[t][0], xcat)
        prod[...] = begun[t] + total if early else total

    def combine(first, sends, prod):
        at = anchors or [factors[group] for _, _, group in sends]
        for r in range(0, tile, 8):
            for col in range(0, TOKENS, 256):
                terms = [
                    prod[(p % 4) * tile + r : (p % 4) * tile + r + 8, (p // 4) * TOKENS + col : (p // 4) * TOKENS + col + 256]
                    for p in range(8)
                ]
                for (d, slot, _), anchor in zip(sends, at):
                    total = terms[7]
                    for p in range(6, -1, -1):
                        total = total * anchor + terms[p]
                    outs[d][slot, first + r : first + r + 8, col : col + 256] = total.astype(BF16)

    multiply(0, prods[0])
    for t in range(4):
        if t < 3:
            multiply(t + 1, prods[(t + 1) % 2])
        combine(plan[t][2], plan[t][3], prods[t % 2])


def product(family, pieces, xd, where, factors, order, begun):
    rows = rows_of(family)
    planes = planes_of(family)
    pieces = [p.reshape(-1, rows, 128) for p in (pieces[4:] if begun else pieces)]
    xd = xd.reshape(4, planes - 4, rows, 128)
    flops = 2 * 4 * rows * 1024 * 1024
    args = [*pieces, xd, *begun]
    out = pl.pallas_call(
        functools.partial(product_kernel, family),
        out_shape=[jax.ShapeDtypeStruct(OUT[family], BF16)] * 4 + [jax.ShapeDtypeStruct((1,), jnp.int32)],
        in_specs=[SMEM, SMEM, SMEM] + [VMEM] * len(args),
        out_specs=[VMEM] * 4 + [SMEM],
        scratch_shapes=[pltpu.VMEM((512 if begun else 1024, 1024), BF16)]
        + [pltpu.VMEM((4 * TILE[family], 1024), F32)] * 2,
        cost_estimate=pl.CostEstimate(flops=2 * flops, bytes_accessed=8 << 20, transcendentals=0),
        compiler_params=pltpu.CompilerParams(vmem_limit_bytes=12 << 20),
    )(where, factors, order, *args)
    return out[:4], out[4]


def cut_kernel(index, where, *refs):
    parts, outs = refs[:4], refs[4:]
    pos = tuple(where[i] for i in range(4))
    for d, out in enumerate(outs):
        at = index(pos, d)
        total = parts[0][at].astype(F32)
        for part in parts[1:]:
            total = total + part[at].astype(F32)
        out[...] = total.astype(out.dtype)


def sum_and_cut(parts, where, index, shape, sends):
    size = int(np.prod(parts[0].shape))
    return pl.pallas_call(
        functools.partial(cut_kernel, index),
        out_shape=[jax.ShapeDtypeStruct(shape, F32)] + [jax.ShapeDtypeStruct(shape, BF16)] * sends,
        in_specs=[SMEM] + [VMEM] * 4,
        out_specs=[VMEM] * (sends + 1),
        cost_estimate=pl.CostEstimate(flops=size * 4, bytes_accessed=size * 12, transcendentals=0),
        compiler_params=pltpu.CompilerParams(vmem_limit_bytes=8 << 20),
    )(where, *parts)


def exchange(parts, axis):
    arrived = {0: parts[0]}
    for d in (2, 1, 3):
        if d < len(parts):
            arrived[d] = flip(parts[d], axis, d)
    return [arrived[d] for d in range(len(parts))]


def close_kernel(*refs):
    fy, out = refs[:4], refs[4]
    total = fy[0][...]
    for part in fy[1:]:
        total = total + part[...].astype(F32)
    out[0, AT_Y : AT_Y + ROWS_Y, :] = total


def final_kernel(where, *refs):
    fx, fz, out, rows_x, rows_z, sem = refs[:4], refs[4:6], *refs[7:]
    x, zl, quarter, half = where[0], where[2], ROWS_X // 4, ROWS_Z // 2
    for d in range(2):
        rows_z[pl.ds(pl.multiple_of((zl ^ d) * half, 16), half), :] = fz[d][...].astype(F32)
    for d in range(4):
        rows_x[pl.ds(pl.multiple_of((x ^ d) * quarter, 16), quarter), :] = fx[d][...].astype(F32)
    copies = [
        pltpu.make_async_copy(rows_z, out.at[0, pl.ds(AT_Z, ROWS_Z)], sem.at[0]),
        pltpu.make_async_copy(rows_x, out.at[0, pl.ds(0, ROWS_X)], sem.at[1]),
    ]
    for copy in copies:
        copy.start()
    for copy in copies:
        copy.wait()


def per_device(weight, activation, points):
    x, y, c = lax.axis_index("x"), lax.axis_index("y"), lax.axis_index("c")
    zl, zh = lax.axis_index("zl"), lax.axis_index("zh")
    where = jnp.stack([x, y, zl, zh, c]).astype(jnp.int32)
    factors = (points + 1).astype(F32) / 8
    view = weight.reshape(4, 2, 4, 2, 512, 128)

    pieces, parts, order = {}, {}, where
    for family in FAMILIES:
        sent, order = pack(family, view, activation, order)
        same = exchange(sent[:4], family)
        cross = {}
        for d in range(4):
            cross[d] = flip(sent[4 + d], family, d, 1)
        pieces[family] = same + [cross[d] for d in range(4)]
    order, shared = order[:1], {}

    def share(family, order):
        xd, order = relay(family, pieces[family][:4], order)
        shared[family] = flip(xd, "c", 0, 1)
        return order

    begun = {family: [] for family in FAMILIES}

    def early(family, order):
        product_so_far, order = begin(family, pieces[family][:4], where, order)
        begun[family] = [product_so_far]
        return order

    order = early(FAMILIES[0], share(FAMILIES[0], order))
    order = early(FAMILIES[1], share(FAMILIES[1], order))
    for family in FAMILIES:
        if family == FAMILIES[2]:
            order = share(family, order)
        parts[family], order = product(
            family, pieces[family], shared[family], where, factors, order, begun[family]
        )

    px = exchange(parts["x"], "z")
    py = exchange(parts["y"], "x")
    pz = exchange(parts["z"], "y")
    px = [p.reshape(4, 4, ROWS_X // 4, TOKENS) for p in px]
    py = [p.reshape(2, 2, ROWS_Y, TOKENS) for p in py]
    pz = [p.reshape(4, 2, ROWS_Z // 2, TOKENS) for p in pz]
    px = sum_and_cut(
        px, where, lambda pos, d: (slice(None), pos[1] ^ d), (4, ROWS_X // 4, TOKENS), 3)
    py = sum_and_cut(
        py, where, lambda pos, d: (pos[2] ^ (d & 1), pos[3] ^ (d >> 1)), (ROWS_Y, TOKENS), 3)
    pz = sum_and_cut(pz, where, lambda pos, d: (pos[0] ^ d,), (2, ROWS_Z // 2, TOKENS), 3)
    px = exchange(px, "y")
    py = exchange(py, "z")
    pz = exchange(pz, "x")
    px = sum_and_cut(px, where, lambda pos, d: (pos[0] ^ d,), (ROWS_X // 4, TOKENS), 3)
    pz = sum_and_cut(pz, where, lambda pos, d: (pos[2] ^ d,), (ROWS_Z // 2, TOKENS), 1)
    px = exchange(px, "x")
    pz = exchange(pz, "z")
    out = pl.pallas_call(
        close_kernel,
        out_shape=jax.ShapeDtypeStruct((1, 512, TOKENS), F32),
        in_specs=[VMEM] * 4,
        out_specs=VMEM,
        cost_estimate=pl.CostEstimate(flops=1 << 20, bytes_accessed=3 << 20, transcendentals=0),
        compiler_params=pltpu.CompilerParams(vmem_limit_bytes=8 << 20),
        name="close",
    )(*py)
    return pl.pallas_call(
        final_kernel,
        out_shape=jax.ShapeDtypeStruct((1, 512, TOKENS), F32),
        in_specs=[SMEM] + [VMEM] * 6 + [HBM],
        out_specs=HBM,
        input_output_aliases={7: 0},
        scratch_shapes=[
            pltpu.VMEM((ROWS_X, TOKENS), F32),
            pltpu.VMEM((ROWS_Z, TOKENS), F32),
            pltpu.SemaphoreType.DMA((2,)),
        ],
        cost_estimate=pl.CostEstimate(flops=1 << 16, bytes_accessed=1 << 19, transcendentals=0),
        compiler_params=pltpu.CompilerParams(vmem_limit_bytes=4 << 20),
        name="final",
    )(where, *px, *pz, out)


def solution(mesh):
    split = Mesh(mesh.devices.reshape(4, 2, 2, 4, 2), AXES)
    grp, mem = ("x", "zl"), ("zh", "y", "c")
    placed = (P(None, None, grp + mem), P(None, grp + mem, None), P())
    return jax.shard_map(per_device, mesh=split, in_specs=placed, out_specs=P(grp, mem, None), check_vma=False)
```
